32 devices in a mesh: dp: 2 (over x), tp: 4 (over z), cp: 4 (over y, core).
Axes of the slice: x: 2, y: 2, z: 4, core: 2. Of those that a mesh axis runs over, the one named last changes fastest.
Arguments:
- x_in: bfloat16 [8192, 2048], P(('dp', 'cp', 'tp')), parts along dimension 0
- w_query: bfloat16 [2048, 32, 64], P(None, 'tp')
- w_key: bfloat16 [2048, 8, 64], P(None, 'tp')
- w_value: bfloat16 [2048, 8, 64], P(None, 'tp')
- w_out: bfloat16 [32, 64, 2048], P('tp')
- d_out: bfloat16 [8192, 2048], P(('dp', 'cp', 'tp')), parts along dimension 0
Outputs:
- output 1: bfloat16 [8192, 2048], P(('dp', 'cp', 'tp')), parts along dimension 0
- output 2: bfloat16 [8192, 2048], P(('dp', 'cp', 'tp')), parts along dimension 0
- output 3: bfloat16 [8, 2048, 32, 64], P(('dp', 'cp'), None, 'tp'), parts along dimension 0
- output 4: bfloat16 [8, 2048, 8, 64], P(('dp', 'cp'), None, 'tp'), parts along dimension 0
- output 5: bfloat16 [8, 2048, 8, 64], P(('dp', 'cp'), None, 'tp'), parts along dimension 0
- output 6: bfloat16 [8, 32, 64, 2048], P(('dp', 'cp'), 'tp'), parts along dimension 0
There are 2 independent parts. The reference program is written for one: setup_inputs(seed, part) draws one part's arguments, and reference() takes and returns one part's arrays. A program takes and returns all parts, laid end to end along the dimension named above; an argument that names none is the same for every part.
All inputs are finite; a program needn't handle non-finite values.
Results may differ from the reference program's by a relative error of at most 0.0111607.
Values are sent between devices in bfloat16 or wider.
A program may use at most 1 GiB of HBM per device.

```python
import math
import jax
import jax.numpy as jnp
from jax import lax

MODEL_DIM = 2048
NUM_HEADS = 32
NUM_KV_HEADS = 8
HEAD_DIM = 64
SEQ_LEN = 4096
SEQ_SHARDS = 4
QUERY_BLOCK = 32


def setup_inputs(seed: int = 0, part: int = 0) -> dict:
    shared_keys = jax.random.split(jax.random.key(seed), 4)
    part_keys = jax.random.split(jax.random.fold_in(jax.random.key(seed), part), 2)
    logit_gain = 1.6
    in_scale = 1.0 / math.sqrt(MODEL_DIM)
    x_in = jax.random.normal(part_keys[0], (SEQ_LEN, MODEL_DIM), jnp.float32)
    w_query = jax.random.normal(shared_keys[0], (MODEL_DIM, NUM_HEADS, HEAD_DIM), jnp.float32) * (logit_gain * in_scale)
    w_key = jax.random.normal(shared_keys[1], (MODEL_DIM, NUM_KV_HEADS, HEAD_DIM), jnp.float32) * (logit_gain * in_scale)
    w_value = jax.random.normal(shared_keys[2], (MODEL_DIM, NUM_KV_HEADS, HEAD_DIM), jnp.float32) * in_scale
    w_out = jax.random.normal(shared_keys[3], (NUM_HEADS, HEAD_DIM, MODEL_DIM), jnp.float32) / math.sqrt(NUM_HEADS * HEAD_DIM)
    d_out = jax.random.normal(part_keys[1], (SEQ_LEN, MODEL_DIM), jnp.float32)
    return {"x_in": x_in.astype(jnp.bfloat16), "w_query": w_query.astype(jnp.bfloat16), "w_key": w_key.astype(jnp.bfloat16), "w_value": w_value.astype(jnp.bfloat16), "w_out": w_out.astype(jnp.bfloat16), "d_out": d_out.astype(jnp.bfloat16)}


def stored_positions():
    half_rows = SEQ_LEN // (2 * SEQ_SHARDS)
    row_ids = jnp.arange(SEQ_LEN, dtype=jnp.int32)
    shard_id = row_ids // (2 * half_rows)
    within = row_ids % (2 * half_rows)
    return jnp.where(within < half_rows, shard_id * half_rows + within, (2 * SEQ_SHARDS - 1 - shard_id) * half_rows + within - half_rows)


def reference(x_in, w_query, w_key, w_value, w_out, d_out):
    groups = NUM_HEADS // NUM_KV_HEADS
    attn_scale = 1.0 / math.sqrt(HEAD_DIM)
    n_blocks = SEQ_LEN // QUERY_BLOCK
    shard_rows = SEQ_LEN // SEQ_SHARDS
    q_cols = NUM_HEADS * HEAD_DIM
    kv_cols = NUM_KV_HEADS * HEAD_DIM
    wq_flat = w_query.reshape(MODEL_DIM, q_cols)
    wk_flat = w_key.reshape(MODEL_DIM, kv_cols)
    wv_flat = w_value.reshape(MODEL_DIM, kv_cols)
    wo_flat = w_out.reshape(q_cols, MODEL_DIM)
    q_flat = jnp.dot(x_in, wq_flat, preferred_element_type=jnp.float32).astype(jnp.bfloat16)
    k_flat = jnp.dot(x_in, wk_flat, preferred_element_type=jnp.float32).astype(jnp.bfloat16)
    v_flat = jnp.dot(x_in, wv_flat, preferred_element_type=jnp.float32).astype(jnp.bfloat16)
    positions = stored_positions()
    k_heads = k_flat.reshape(SEQ_LEN, NUM_KV_HEADS, HEAD_DIM).astype(jnp.float32)
    v_heads = v_flat.reshape(SEQ_LEN, NUM_KV_HEADS, HEAD_DIM).astype(jnp.float32)
    q_blocks = q_flat.reshape(n_blocks, QUERY_BLOCK, NUM_KV_HEADS, groups, HEAD_DIM)
    pos_blocks = positions.reshape(n_blocks, QUERY_BLOCK)

    def block_scores(q_blk, pos_blk):
        scores = jnp.einsum("qhgd,khd->qhgk", q_blk.astype(jnp.float32), k_heads) * attn_scale
        visible = pos_blk[:, None, None, None] >= positions[None, None, None, :]
        return jnp.where(visible, scores, -jnp.inf)

    def forward_block(block_in):
        q_blk, pos_blk = block_in
        scores = block_scores(q_blk, pos_blk)
        row_max = jnp.max(scores, axis=-1)
        prob_mat = jnp.exp(scores - row_max[..., None])
        row_sum = jnp.sum(prob_mat, axis=-1)
        pv_sum = jnp.einsum("qhgk,khd->qhgd", prob_mat.astype(jnp.bfloat16).astype(jnp.float32), v_heads)
        out_blk = (pv_sum / row_sum[..., None]).astype(jnp.bfloat16)
        return out_blk, row_max + jnp.log(row_sum)

    o_blocks, lse_blocks = lax.map(forward_block, (q_blocks, pos_blocks))
    o_flat = o_blocks.reshape(SEQ_LEN, q_cols)
    y_out = jnp.dot(o_flat, wo_flat, preferred_element_type=jnp.float32).astype(jnp.bfloat16)

    do_flat = jnp.dot(d_out, wo_flat.T, preferred_element_type=jnp.float32).astype(jnp.bfloat16)
    do_blocks = do_flat.reshape(n_blocks, QUERY_BLOCK, NUM_KV_HEADS, groups, HEAD_DIM)
    dot_blocks = jnp.sum(do_blocks.astype(jnp.float32) * o_blocks.astype(jnp.float32), axis=-1)

    def backward_block(grad_carry, block_in):
        dk_acc, dv_acc = grad_carry
        q_blk, pos_blk, lse_blk, do_blk, dot_blk = block_in
        scores = block_scores(q_blk, pos_blk)
        prob_mat = jnp.exp(scores - lse_blk[..., None])
        do_wide = do_blk.astype(jnp.float32)
        d_probs = jnp.einsum("qhgd,khd->qhgk", do_wide, v_heads)
        d_scores = (prob_mat * (d_probs - dot_blk[..., None])).astype(jnp.bfloat16).astype(jnp.float32)
        dv_acc = dv_acc + jnp.einsum("qhgk,qhgd->khd", prob_mat.astype(jnp.bfloat16).astype(jnp.float32), do_wide)
        dk_acc = dk_acc + jnp.einsum("qhgk,qhgd->khd", d_scores, q_blk.astype(jnp.float32)) * attn_scale
        dq_blk = jnp.einsum("qhgk,khd->qhgd", d_scores, k_heads) * attn_scale
        return (dk_acc, dv_acc), dq_blk.astype(jnp.bfloat16)

    zero_kv = jnp.zeros((SEQ_LEN, NUM_KV_HEADS, HEAD_DIM), jnp.float32)
    grad_kv, dq_blocks = lax.scan(backward_block, (zero_kv, zero_kv), (q_blocks, pos_blocks, lse_blocks, do_blocks, dot_blocks))
    dq_flat = dq_blocks.reshape(SEQ_LEN, q_cols)
    dk_flat = grad_kv[0].astype(jnp.bfloat16).reshape(SEQ_LEN, kv_cols)
    dv_flat = grad_kv[1].astype(jnp.bfloat16).reshape(SEQ_LEN, kv_cols)
    dx_sum = (jnp.dot(dq_flat, wq_flat.T, preferred_element_type=jnp.float32)
              + jnp.dot(dk_flat, wk_flat.T, preferred_element_type=jnp.float32)
              + jnp.dot(dv_flat, wv_flat.T, preferred_element_type=jnp.float32))
    grad_x = dx_sum.astype(jnp.bfloat16)
    x_shards = x_in.reshape(SEQ_SHARDS, shard_rows, MODEL_DIM).astype(jnp.float32)
    grad_wq = jnp.einsum("rsm,rsc->rmc", x_shards, dq_flat.reshape(SEQ_SHARDS, shard_rows, q_cols).astype(jnp.float32)).astype(jnp.bfloat16).reshape(SEQ_SHARDS, MODEL_DIM, NUM_HEADS, HEAD_DIM)
    grad_wk = jnp.einsum("rsm,rsc->rmc", x_shards, dk_flat.reshape(SEQ_SHARDS, shard_rows, kv_cols).astype(jnp.float32)).astype(jnp.bfloat16).reshape(SEQ_SHARDS, MODEL_DIM, NUM_KV_HEADS, HEAD_DIM)
    grad_wv = jnp.einsum("rsm,rsc->rmc", x_shards, dv_flat.reshape(SEQ_SHARDS, shard_rows, kv_cols).astype(jnp.float32)).astype(jnp.bfloat16).reshape(SEQ_SHARDS, MODEL_DIM, NUM_KV_HEADS, HEAD_DIM)
    grad_wo = jnp.einsum("rsc,rsm->rcm", o_flat.reshape(SEQ_SHARDS, shard_rows, q_cols).astype(jnp.float32), d_out.reshape(SEQ_SHARDS, shard_rows, MODEL_DIM).astype(jnp.float32)).astype(jnp.bfloat16).reshape(SEQ_SHARDS, NUM_HEADS, HEAD_DIM, MODEL_DIM)
    return y_out, grad_x, grad_wq, grad_wk, grad_wv, grad_wo
```

```python
import functools

import jax
import jax.numpy as jnp
from jax import lax
from jax.experimental import pallas as pl
from jax.experimental.pallas import tpu as pltpu
from jax.sharding import PartitionSpec as P

ROW_SPEC = P(("dp", "cp", "tp"), None)
HEAD_SPEC = P(None, "tp", None)
OUT_W_SPEC = P("tp", None, None)
GRAD_SPEC = P(("dp", "cp"), None, "tp", None)
GRAD_OUT_SPEC = P(("dp", "cp"), "tp", None, None)
TN = (((0,), (0,)), ((), ()))
NT = (((1,), (1,)), ((), ()))
TT = (((0,), (1,)), ((), ()))
F32 = jnp.float32
BF16 = jnp.bfloat16


def mm(lhs, rhs, dims=(((1,), (0,)), ((), ()))):
    return lax.dot_general(lhs, rhs, dims, preferred_element_type=F32)


def chunk_offset(chunk, rank, n_shards, half):
    shard = jnp.where(chunk < n_shards, chunk, 2 * n_shards - 1 - chunk)
    upper = jnp.where(chunk < n_shards, 0, half)
    return pl.multiple_of(lax.bitwise_xor(shard, rank) * (2 * half) + upper, half)


def forward_kernel(n_shards, groups, d, half, rank_ref, qt_ref, kv_ref, kvt_ref, ot_ref, lse_ref, q_pad, m_s, l_s, acc_s):
    rank = rank_ref[0]
    kv_heads = qt_ref.shape[0] // (groups * d)
    kw = kv_heads * d
    n_rows = qt_ref.shape[1]
    sub = half // 2
    q_pad[...] = jnp.zeros_like(q_pad)
    for h in range(kv_heads):
        for g in range(groups):
            q_pad[h * groups + g, h * d:(h + 1) * d, :] = qt_ref[(h * groups + g) * d:(h * groups + g + 1) * d, :]

    def update(h, g, q_start, q_lo, q_len, k_off, k_len, masked):
        cols = slice(q_lo, q_lo + q_len)
        q_blk = q_pad[h * groups + g, :, q_start + q_lo:q_start + q_lo + q_len]
        scores = mm(kv_ref[pl.ds(k_off, k_len), :kw], q_blk)
        if masked:
            k_id = lax.broadcasted_iota(jnp.int32, scores.shape, 0)
            q_id = lax.broadcasted_iota(jnp.int32, scores.shape, 1)
            scores = jnp.where(q_id >= k_id, scores, -jnp.inf)
        m_old = m_s[g:g + 1, cols]
        m_new = jnp.maximum(m_old, jnp.max(scores, axis=0, keepdims=True))
        prob = jnp.exp(scores - m_new)
        factor = jnp.exp(m_old - m_new)
        m_s[g:g + 1, cols] = m_new
        l_s[g:g + 1, cols] = l_s[g:g + 1, cols] * factor + jnp.sum(prob, axis=0, keepdims=True)
        pv = mm(kvt_ref[kw + h * d:kw + (h + 1) * d, pl.ds(k_off, k_len)], prob.astype(BF16))
        acc_s[g * d:(g + 1) * d, cols] = acc_s[g * d:(g + 1) * d, cols] * factor + pv

    for h in range(kv_heads):
        for q_half in range(2):
            q_start = q_half * half
            n_full = rank if q_half == 0 else 2 * n_shards - 1 - rank
            m_s[...] = jnp.full_like(m_s, -jnp.inf)
            l_s[...] = jnp.zeros_like(l_s)
            acc_s[...] = jnp.zeros_like(acc_s)
            off = chunk_offset(n_full, rank, n_shards, half)
            for g in range(groups):
                update(h, g, q_start, 0, half, off, sub, True)
                update(h, g, q_start, sub, sub, pl.multiple_of(off + sub, sub), sub, True)

            def full_block(chunk, carry):
                k_off = chunk_offset(chunk, rank, n_shards, half)
                for g in range(groups):
                    update(h, g, q_start, 0, half, k_off, half, False)
                return carry

            lax.fori_loop(0, n_full, full_block, 0)
            for g in range(groups):
                j = h * groups + g
                l_row = l_s[g:g + 1, :]
                ot_ref[j * d:(j + 1) * d, q_start:q_start + half] = (acc_s[g * d:(g + 1) * d, :] / l_row).astype(BF16)
                lse_ref[j:j + 1, q_start:q_start + half] = m_s[g:g + 1, :] + jnp.log(l_row)


def backward_kernel(n_shards, groups, d, half, h, kv_heads, rank_ref, qt_ref, dot_ref, ot_ref, lse_ref, kv_ref, kt_ref,
                    dqt_ref, dkv_ref, q_pad, do_pad, delta_s, dq_s):
    rank = rank_ref[0]
    kw = kv_heads * d
    sub = half // 2
    q_pad[...] = jnp.zeros_like(q_pad)
    do_pad[...] = jnp.zeros_like(do_pad)
    for g in range(groups):
        rows = slice(g * d, (g + 1) * d)
        q_pad[g, h * d:(h + 1) * d, :] = qt_ref[rows, :]
        do_pad[g, h * d:(h + 1) * d, :] = dot_ref[rows, :]
        delta_s[g:g + 1, :] = jnp.sum(dot_ref[rows, :].astype(F32) * ot_ref[rows, :].astype(F32), axis=0, keepdims=True)
    dkv_ref[...] = jnp.zeros_like(dkv_ref)

    def update(q_start, q_lo, q_len, k_off, k_len, masked):
        lo = q_start + q_lo
        cols = slice(lo, lo + q_len)
        k_blk = kv_ref[pl.ds(k_off, k_len), :kw]
        v_blk = kv_ref[pl.ds(k_off, k_len), kw:]
        dk_sum, dv_sum = None, None
        for g in range(groups):
            rows = slice(g * d, (g + 1) * d)
            scores = mm(k_blk, q_pad[g, :, cols])
            prob = jnp.exp(scores - lse_ref[g:g + 1, cols])
            if masked:
                k_id = lax.broadcasted_iota(jnp.int32, scores.shape, 0)
                q_id = lax.broadcasted_iota(jnp.int32, scores.shape, 1)
                prob = jnp.where(q_id >= k_id, prob, 0.0)
            d_prob = mm(v_blk, do_pad[g, :, cols])
            d_score = (prob * (d_prob - delta_s[g:g + 1, cols])).astype(BF16)
            dv = mm(dot_ref[rows, cols], prob.astype(BF16), NT)
            dk = mm(qt_ref[rows, cols], d_score, NT)
            dk_sum = dk if dk_sum is None else dk_sum + dk
            dv_sum = dv if dv_sum is None else dv_sum + dv
            dq_s[rows, q_lo:q_lo + q_len] += mm(kt_ref[h * d:(h + 1) * d, pl.ds(k_off, k_len)], d_score)
        dkv_ref[:d, pl.ds(k_off, k_len)] += dk_sum
        dkv_ref[d:, pl.ds(k_off, k_len)] += dv_sum

    for q_half in range(2):
        q_start = q_half * half
        n_full = rank if q_half == 0 else 2 * n_shards - 1 - rank
        dq_s[...] = jnp.zeros_like(dq_s)
        off = chunk_offset(n_full, rank, n_shards, half)
        update(q_start, 0, half, off, sub, True)
        update(q_start, sub, sub, pl.multiple_of(off + sub, sub), sub, True)

        def full_block(chunk, carry):
            update(q_start, 0, half, chunk_offset(chunk, rank, n_shards, half), half, False)
            return carry

        lax.fori_loop(0, n_full, full_block, 0)
        dqt_ref[:, q_start:q_start + half] = (dq_s[...] * (d ** -0.5)).astype(BF16)


VMEM = pl.BlockSpec(memory_space=pltpu.VMEM)
SMEM = pl.BlockSpec(memory_space=pltpu.SMEM)


def attention_forward(rank_arr, qt, kv_all, kvt_all, n_shards, groups, d, interpret=False):
    heads = qt.shape[0] // d
    n_rows = qt.shape[1]
    half = n_rows // 2
    kw = kv_all.shape[1] // 2
    pairs = heads * n_rows * n_rows * n_shards // 2
    return pl.pallas_call(
        functools.partial(forward_kernel, n_shards, groups, d, half),
        out_shape=(jax.ShapeDtypeStruct(qt.shape, BF16), jax.ShapeDtypeStruct((heads, n_rows), F32)),
        in_specs=[SMEM, VMEM, VMEM, VMEM],
        out_specs=(VMEM, VMEM),
        scratch_shapes=[pltpu.VMEM((heads, kw, n_rows), BF16), pltpu.VMEM((groups, half), F32), pltpu.VMEM((groups, half), F32),
                        pltpu.VMEM((groups * d, half), F32)],
        cost_estimate=pl.CostEstimate(flops=16 * d * pairs, bytes_accessed=6 << 20, transcendentals=pairs),
        compiler_params=pltpu.CompilerParams(vmem_limit_bytes=40 << 20),
        name="attention_forward",
        interpret=interpret,
    )(rank_arr, qt, kv_all, kvt_all)


def attention_backward(rank_arr, qt, dot, ot, lse, kv_all, kt_all, h, kv_heads, n_shards, groups, d, interpret=False):
    n_rows = qt.shape[1]
    half = n_rows // 2
    kw = kv_all.shape[1] // 2
    pairs = groups * n_rows * n_rows * n_shards // 2
    return pl.pallas_call(
        functools.partial(backward_kernel, n_shards, groups, d, half, h, kv_heads),
        out_shape=(jax.ShapeDtypeStruct(qt.shape, BF16), jax.ShapeDtypeStruct((2 * d, kv_all.shape[0]), F32)),
        in_specs=[SMEM] + [VMEM] * 6,
        out_specs=(VMEM, VMEM),
        scratch_shapes=[pltpu.VMEM((groups, kw, n_rows), BF16), pltpu.VMEM((groups, kw, n_rows), BF16),
                        pltpu.VMEM((groups, n_rows), F32), pltpu.VMEM((groups * d, half), F32)],
        cost_estimate=pl.CostEstimate(flops=40 * d * pairs, bytes_accessed=8 << 20, transcendentals=pairs),
        compiler_params=pltpu.CompilerParams(vmem_limit_bytes=40 << 20),
        name=f"attention_backward_{h}",
        interpret=interpret,
    )(rank_arr, qt, dot, ot, lse, kv_all, kt_all)


def solution(mesh, interpret=False):
    n_cp, n_tp, n_dp = mesh.shape["cp"], mesh.shape["tp"], mesh.shape["dp"]

    def swap(arr, axis, bit):
        size = mesh.shape[axis]
        return lax.ppermute(arr, axis, [(i, i ^ bit) for i in range(size)])

    def device_fn(x_blk, w_query, w_key, w_value, w_out, dy_blk):
        rank = lax.axis_index("cp")
        model, q_heads, d = w_query.shape
        kv_heads = w_key.shape[1]
        groups = q_heads // kv_heads
        gd = groups * d
        rank_arr = rank.astype(jnp.int32).reshape(1)
        wq = w_query.reshape(model, q_heads * d)
        wk = w_key.reshape(model, kv_heads * d)
        wv = w_value.reshape(model, kv_heads * d)
        wkv = jnp.concatenate([wk, wv], axis=1)
        wo = w_out.reshape(q_heads * d, model)

        x_rows = lax.all_gather(x_blk, "tp", axis=0, tiled=True)
        n_rows = x_rows.shape[0]
        kv_own = mm(x_rows, wkv).astype(BF16)
        qt = mm(wq, x_rows, TT).astype(BF16) * BF16(d ** -0.5)

        kv_core = swap(kv_own, "cp", 1)
        kv_far = swap(kv_own, "cp", 2)
        kv_diag = swap(kv_far, "cp", 1)
        kv_all = jnp.concatenate([kv_own, kv_core, kv_far, kv_diag], axis=0)
        kvt_all = kv_all.T

        ot, lse = attention_forward(rank_arr, qt, kv_all, kvt_all, n_cp, groups, d, interpret)

        dy_rows = lax.all_gather(dy_blk, "tp", axis=0, tiled=True)
        dy_rows, ot, lse = lax.optimization_barrier((dy_rows, ot, lse))
        dot = mm(wo, dy_rows, NT).astype(BF16)

        n_plane = n_dp * n_cp
        plane = lax.axis_index("dp") * n_cp + rank
        w_heads = jnp.concatenate([part for h in range(kv_heads) for part in
                                   (wq[:, h * gd:(h + 1) * gd], wk[:, h * d:(h + 1) * d], wv[:, h * d:(h + 1) * d])], axis=1)
        n_in = w_heads.shape[1] // n_plane
        n_out = wo.shape[0] // n_plane
        w_in_piece = lax.dynamic_slice(w_heads, (0, plane * n_in), (model, n_in)).T
        wo_piece = lax.dynamic_slice(wo, (plane * n_out, 0), (n_out, model))
        wo_piece, w_in_piece, _ = lax.optimization_barrier((wo_piece, w_in_piece, qt))
        wo_full = lax.all_gather(wo_piece, ("dp", "tp", "cp"), axis=0, tiled=True)
        w_in_full = lax.all_gather(w_in_piece, ("dp", "tp", "cp"), axis=0, tiled=True)

        def exchange(arr_t):
            feats = arr_t.shape[0]
            split = arr_t.reshape(feats, n_tp, n_rows // n_tp).transpose(1, 0, 2)
            return lax.all_to_all(split, "tp", 0, 0, tiled=True)

        def gathered_order(parts):
            feats, rows = parts.shape[1:]
            piece = feats // n_plane
            return parts.reshape(n_tp, n_dp, n_cp, piece, rows).transpose(1, 0, 2, 3, 4).reshape(n_tp * feats, rows)

        o_own = gathered_order(exchange(ot))
        y_blk = mm(o_own, wo_full, TN).astype(BF16)

        dq_parts, dk_parts, dv_parts, moved = [], [], [], []
        for h in range(kv_heads):
            rows = slice(h * gd, (h + 1) * gd)
            dqt, dkv = attention_backward(rank_arr, qt[rows], dot[rows], ot[rows], lse[h * groups:(h + 1) * groups],
                                          kv_all, kvt_all[:kv_heads * d], h, kv_heads, n_cp, groups, d, interpret)
            slots = [dkv[:, j * n_rows:(j + 1) * n_rows] for j in range(n_cp)]
            near = swap(jnp.concatenate([slots[1], slots[3]], axis=1), "cp", 1)
            far = swap(slots[2] + near[:, n_rows:], "cp", 2)
            dkv_own = (slots[0] + near[:, :n_rows] + far).astype(BF16)
            dq_parts.append(dqt)
            dk_parts.append(dkv_own[:d])
            dv_parts.append(dkv_own[d:])
            moved.append(exchange(jnp.concatenate([dqt, dkv_own], axis=0)))
        grads_own = gathered_order(jnp.concatenate(moved, axis=1))
        dx_blk = mm(grads_own, w_in_full, TN).astype(BF16)

        dqt = jnp.concatenate(dq_parts, axis=0)
        dkt = jnp.concatenate(dk_parts, axis=0)
        dvt = jnp.concatenate(dv_parts, axis=0)
        grad_wq = mm(x_rows, dqt, TT).astype(BF16).reshape(model, q_heads, d)
        grad_wk = mm(x_rows, dkt, TT).astype(BF16).reshape(model, kv_heads, d)
        grad_wv = mm(x_rows, dvt, TT).astype(BF16).reshape(model, kv_heads, d)
        grad_wo = mm(ot, dy_rows).astype(BF16).reshape(q_heads, d, model)
        return y_blk, dx_blk, grad_wq[None], grad_wk[None], grad_wv[None], grad_wo[None]

    return jax.shard_map(device_fn, mesh=mesh,
                         in_specs=(ROW_SPEC, HEAD_SPEC, HEAD_SPEC, HEAD_SPEC, OUT_W_SPEC, ROW_SPEC),
                         out_specs=(ROW_SPEC, ROW_SPEC, GRAD_SPEC, GRAD_SPEC, GRAD_SPEC, GRAD_OUT_SPEC),
                         check_vma=False)
```

```python
import functools

import jax
import jax.numpy as jnp
from jax import lax
from jax.experimental import pallas as pl
from jax.experimental.pallas import tpu as pltpu
from jax.sharding import PartitionSpec as P

ROW_SPEC = P(("dp", "cp", "tp"), None)
HEAD_SPEC = P(None, "tp", None)
OUT_W_SPEC = P("tp", None, None)
GRAD_SPEC = P(("dp", "cp"), None, "tp", None)
GRAD_OUT_SPEC = P(("dp", "cp"), "tp", None, None)
TN = (((0,), (0,)), ((), ()))
NT = (((1,), (1,)), ((), ()))
F32 = jnp.float32
BF16 = jnp.bfloat16


def mm(lhs, rhs, dims=(((1,), (0,)), ((), ()))):
    return lax.dot_general(lhs, rhs, dims, preferred_element_type=F32)


def chunk_offset(chunk, rank, n_shards, half):
    shard = jnp.where(chunk < n_shards, chunk, 2 * n_shards - 1 - chunk)
    upper = jnp.where(chunk < n_shards, 0, half)
    return pl.multiple_of(lax.bitwise_xor(shard, rank) * (2 * half) + upper, half)


def forward_kernel(n_shards, groups, d, half, h, kv_heads, rank_ref, qt_ref, kv_ref, ot_ref, lse_ref, kt_ref, q_pad, vt_s, m_s, l_s, acc_s):
    rank = rank_ref[0]
    kw = kv_heads * d
    sub = half // 2
    q_pad[...] = jnp.zeros_like(q_pad)
    for g in range(groups):
        q_pad[g, h * d:(h + 1) * d, :] = qt_ref[(h * groups + g) * d:(h * groups + g + 1) * d, :]

    def transpose_chunk(i, carry):
        rows = pl.ds(pl.multiple_of(i * half, half), half)
        kt_ref[:, rows] = kv_ref[rows, :kw].T[h * d:(h + 1) * d, :]
        vt_s[:, rows] = kv_ref[rows, kw:].T[h * d:(h + 1) * d, :]
        return carry

    lax.fori_loop(0, kv_ref.shape[0] // half, transpose_chunk, 0)

    def update(g, q_start, q_lo, q_len, k_off, k_len, masked):
        cols = slice(q_lo, q_lo + q_len)
        scores = mm(kv_ref[pl.ds(k_off, k_len), :kw], q_pad[g, :, q_start + q_lo:q_start + q_lo + q_len])
        if masked:
            k_id = lax.broadcasted_iota(jnp.int32, scores.shape, 0)
            q_id = lax.broadcasted_iota(jnp.int32, scores.shape, 1)
            scores = jnp.where(q_id >= k_id, scores, -jnp.inf)
        m_old = m_s[g:g + 1, cols]
        m_new = jnp.maximum(m_old, jnp.max(scores, axis=0, keepdims=True))
        prob = jnp.exp(scores - m_new)
        factor = jnp.exp(m_old - m_new)
        m_s[g:g + 1, cols] = m_new
        l_s[g:g + 1, cols] = l_s[g:g + 1, cols] * factor + jnp.sum(prob, axis=0, keepdims=True)
        pv = mm(vt_s[:, pl.ds(k_off, k_len)], prob.astype(BF16))
        acc_s[g * d:(g + 1) * d, cols] = acc_s[g * d:(g + 1) * d, cols] * factor + pv

    for q_half in range(2):
        q_start = q_half * half
        n_full = rank if q_half == 0 else 2 * n_shards - 1 - rank
        m_s[...] = jnp.full_like(m_s, -jnp.inf)
        l_s[...] = jnp.zeros_like(l_s)
        acc_s[...] = jnp.zeros_like(acc_s)
        off = chunk_offset(n_full, rank, n_shards, half)
        for g in range(groups):
            update(g, q_start, 0, half, off, sub, True)
        for g in range(groups):
            update(g, q_start, sub, sub, pl.multiple_of(off + sub, sub), sub, True)

        def full_block(chunk, carry):
            k_off = chunk_offset(chunk, rank, n_shards, half)
            for g in range(groups):
                update(g, q_start, 0, half, k_off, half, False)
            return carry

        lax.fori_loop(0, n_full, full_block, 0)
        for g in range(groups):
            l_row = l_s[g:g + 1, :]
            ot_ref[g * d:(g + 1) * d, q_start:q_start + half] = (acc_s[g * d:(g + 1) * d, :] / l_row).astype(BF16)
            lse_ref[g:g + 1, q_start:q_start + half] = m_s[g:g + 1, :] + jnp.log(l_row)


def backward_kernel(n_shards, groups, d, half, h, kv_heads, rank_ref, qt_ref, dot_ref, ot_ref, lse_ref, kv_ref, kt_ref,
                    dqt_ref, dkv_ref, q_pad, do_pad, delta_s, dq_s):
    rank = rank_ref[0]
    kw = kv_heads * d
    sub = half // 2
    q_pad[...] = jnp.zeros_like(q_pad)
    do_pad[...] = jnp.zeros_like(do_pad)
    for g in range(groups):
        rows = slice(g * d, (g + 1) * d)
        full = slice((h * groups + g) * d, (h * groups + g + 1) * d)
        q_pad[g, h * d:(h + 1) * d, :] = qt_ref[full, :]
        do_pad[g, h * d:(h + 1) * d, :] = dot_ref[full, :]
        delta_s[g:g + 1, :] = jnp.sum(dot_ref[full, :].astype(F32) * ot_ref[rows, :].astype(F32), axis=0, keepdims=True)
    dkv_ref[...] = jnp.zeros_like(dkv_ref)

    def update(q_start, q_lo, q_len, k_off, k_len, masked):
        lo = q_start + q_lo
        cols = slice(lo, lo + q_len)
        k_blk = kv_ref[pl.ds(k_off, k_len), :kw]
        v_blk = kv_ref[pl.ds(k_off, k_len), kw:]
        dk_sum, dv_sum = None, None
        for g in range(groups):
            rows = slice(g * d, (g + 1) * d)
            full = slice((h * groups + g) * d, (h * groups + g + 1) * d)
            scores = mm(k_blk, q_pad[g, :, cols])
            prob = jnp.exp(scores - lse_ref[g:g + 1, cols])
            if masked:
                k_id = lax.broadcasted_iota(jnp.int32, scores.shape, 0)
                q_id = lax.broadcasted_iota(jnp.int32, scores.shape, 1)
                prob = jnp.where(q_id >= k_id, prob, 0.0)
            d_prob = mm(v_blk, do_pad[g, :, cols])
            d_score = (prob * (d_prob - delta_s[g:g + 1, cols])).astype(BF16)
            dv = mm(dot_ref[full, cols], prob.astype(BF16), NT)
            dk = mm(qt_ref[full, cols], d_score, NT)
            dk_sum = dk if dk_sum is None else dk_sum + dk
            dv_sum = dv if dv_sum is None else dv_sum + dv
            dq_s[rows, q_lo:q_lo + q_len] += mm(kt_ref[:, pl.ds(k_off, k_len)], d_score)
        dkv_ref[:d, pl.ds(k_off, k_len)] += dk_sum
        dkv_ref[d:, pl.ds(k_off, k_len)] += dv_sum

    for q_half in range(2):
        q_start = q_half * half
        n_full = rank if q_half == 0 else 2 * n_shards - 1 - rank
        dq_s[...] = jnp.zeros_like(dq_s)
        off = chunk_offset(n_full, rank, n_shards, half)
        update(q_start, 0, half, off, sub, True)
        update(q_start, sub, sub, pl.multiple_of(off + sub, sub), sub, True)

        def full_block(chunk, carry):
            update(q_start, 0, half, chunk_offset(chunk, rank, n_shards, half), half, False)
            return carry

        lax.fori_loop(0, n_full, full_block, 0)
        dqt_ref[:, q_start:q_start + half] = (dq_s[...] * (d ** -0.5)).astype(BF16)


VMEM = pl.BlockSpec(memory_space=pltpu.VMEM)
SMEM = pl.BlockSpec(memory_space=pltpu.SMEM)


def attention_forward(rank_arr, qt, kv_all, h, kv_heads, n_shards, groups, d, interpret=False):
    n_rows = qt.shape[1]
    half = n_rows // 2
    kw = kv_all.shape[1] // 2
    pairs = groups * n_rows * n_rows * n_shards // 2
    return pl.pallas_call(
        functools.partial(forward_kernel, n_shards, groups, d, half, h, kv_heads),
        out_shape=(jax.ShapeDtypeStruct((groups * d, n_rows), BF16), jax.ShapeDtypeStruct((groups, n_rows), F32),
                   jax.ShapeDtypeStruct((d, kv_all.shape[0]), BF16)),
        in_specs=[SMEM, VMEM, VMEM],
        out_specs=(VMEM, VMEM, VMEM),
        scratch_shapes=[pltpu.VMEM((groups, kw, n_rows), BF16), pltpu.VMEM((d, kv_all.shape[0]), BF16),
                        pltpu.VMEM((groups, half), F32), pltpu.VMEM((groups, half), F32), pltpu.VMEM((groups * d, half), F32)],
        cost_estimate=pl.CostEstimate(flops=32 * d * pairs, bytes_accessed=6 << 20, transcendentals=pairs),
        compiler_params=pltpu.CompilerParams(vmem_limit_bytes=40 << 20),
        name=f"attention_forward_{h}",
        interpret=interpret,
    )(rank_arr, qt, kv_all)


def attention_backward(rank_arr, qt, dot, ot, lse, kv_all, kt, h, kv_heads, n_shards, groups, d, interpret=False):
    n_rows = qt.shape[1]
    half = n_rows // 2
    kw = kv_all.shape[1] // 2
    pairs = groups * n_rows * n_rows * n_shards // 2
    return pl.pallas_call(
        functools.partial(backward_kernel, n_shards, groups, d, half, h, kv_heads),
        out_shape=(jax.ShapeDtypeStruct((groups * d, n_rows), BF16), jax.ShapeDtypeStruct((2 * d, kv_all.shape[0]), F32)),
        in_specs=[SMEM] + [VMEM] * 6,
        out_specs=(VMEM, VMEM),
        scratch_shapes=[pltpu.VMEM((groups, kw, n_rows), BF16), pltpu.VMEM((groups, kw, n_rows), BF16),
                        pltpu.VMEM((groups, n_rows), F32), pltpu.VMEM((groups * d, half), F32)],
        cost_estimate=pl.CostEstimate(flops=40 * d * pairs, bytes_accessed=8 << 20, transcendentals=pairs),
        compiler_params=pltpu.CompilerParams(vmem_limit_bytes=40 << 20),
        name=f"attention_backward_{h}",
        interpret=interpret,
    )(rank_arr, qt, dot, ot, lse, kv_all, kt)


def solution(mesh, interpret=False):
    n_cp, n_tp, n_dp = mesh.shape["cp"], mesh.shape["tp"], mesh.shape["dp"]
    ring = [*range(0, n_tp, 2), *reversed(range(1, n_tp, 2))]
    hop = [(ring[i], ring[(i + 1) % n_tp]) for i in range(n_tp)]
    source = [[ring[(ring.index(z) - s) % n_tp] for z in range(n_tp)] for s in range(n_tp)]
    arrival = [[[source[s][z] for s in range(n_tp)].index(b) for z in range(n_tp)] for b in range(n_tp)]

    def swap(arr, axis, bit):
        return lax.ppermute(arr, axis, [(i, i ^ bit) for i in range(mesh.shape[axis])])

    def pick(table, idx):
        out = jnp.int32(table[0])
        for i, value in enumerate(table[1:], 1):
            out = jnp.where(idx == i, value, out)
        return out

    def device_fn(x_blk, w_query, w_key, w_value, w_out, dy_blk):
        rank = lax.axis_index("cp")
        z = lax.axis_index("tp")
        model, q_heads, d = w_query.shape
        kv_heads = w_key.shape[1]
        groups = q_heads // kv_heads
        gd = groups * d
        blk = x_blk.shape[0]
        n_rows = blk * n_tp
        rank_arr = rank.astype(jnp.int32).reshape(1)
        wqt = w_query.transpose(1, 2, 0).reshape(q_heads * d, model)
        wkt = w_key.transpose(1, 2, 0).reshape(kv_heads * d, model)
        wvt = w_value.transpose(1, 2, 0).reshape(kv_heads * d, model)
        wkvt = jnp.concatenate([wkt, wvt], axis=0)
        wo = w_out.reshape(q_heads * d, model)

        n_plane = n_dp * n_cp
        plane = lax.axis_index("dp") * n_cp + rank
        w_heads = jnp.concatenate([part for h in range(kv_heads) for part in
                                   (wqt[h * gd:(h + 1) * gd], wkt[h * d:(h + 1) * d], wvt[h * d:(h + 1) * d])], axis=0)
        n_in = w_heads.shape[0] // n_plane
        n_out = wo.shape[0] // n_plane
        w_in_piece = lax.dynamic_slice(w_heads, (plane * n_in, 0), (n_in, model))
        wo_piece = lax.dynamic_slice(wo, (plane * n_out, 0), (n_out, model))

        wo_line = lax.all_gather(wo_piece, "tp", axis=0, tiled=True)
        w_in_line = lax.all_gather(w_in_piece, "tp", axis=0, tiled=True)

        def offset(step):
            return pick(source[step], z) * blk

        x_rows = jnp.zeros((n_rows, model), BF16)
        qt = jnp.zeros((q_heads * d, n_rows), BF16)
        kv_blocks, kv_moved = [], []
        held = x_blk

        def cp_exchange(arr):
            near = swap(arr, "cp", 1)
            far = swap(arr, "cp", 2)
            return [arr, near, far, swap(far, "cp", 1)]

        for step in range(n_tp):
            with jax.named_scope(f"x_hop_{step}"):
                following = lax.ppermute(held, "tp", hop) if step < n_tp - 1 else None
            if step == 1:
                wo_line, held = lax.optimization_barrier((wo_line, held))
                wo_full = lax.all_gather(wo_line, ("dp", "cp"), axis=0, tiled=True)
            if step == 2:
                w_in_line, held = lax.optimization_barrier((w_in_line, held))
                w_in_full = lax.all_gather(w_in_line, ("dp", "cp"), axis=0, tiled=True)
            kv_blocks.append(mm(held, wkvt, NT).astype(BF16))
            qt = lax.dynamic_update_slice(qt, mm(wqt, held, NT).astype(BF16) * BF16(d ** -0.5), (0, offset(step)))
            x_rows = lax.dynamic_update_slice(x_rows, held, (offset(step), 0))
            if step == n_tp - 2:
                kv_moved.append(cp_exchange(jnp.stack(kv_blocks)))
            if step == n_tp - 1:
                kv_moved.append(cp_exchange(kv_blocks[-1][None]))
            held = following if following is not None else held
        dy_first, _ = lax.optimization_barrier((dy_blk, held))
        slots = []
        for slot in range(n_cp):
            by_arrival = jnp.concatenate([kv_moved[0][slot], kv_moved[1][slot]], axis=0)
            slots += [lax.dynamic_index_in_dim(by_arrival, pick(arrival[b], z), 0, keepdims=False) for b in range(n_tp)]
        kv_all = jnp.concatenate(slots, axis=0)

        dy_rows = jnp.zeros((n_rows, model), BF16)
        dy_held, dy_blocks = dy_first, [dy_first]
        for step in range(1, n_tp):
            with jax.named_scope(f"dy_hop_{step}"):
                dy_held = lax.ppermute(dy_held, "tp", hop)
            dy_blocks.append(dy_held)

        fwd = []
        for h in range(kv_heads):
            with jax.named_scope(f"fwd_head_{h}"):
                fwd.append(attention_forward(rank_arr, qt, kv_all, h, kv_heads, n_cp, groups, d, interpret))
        ot = jnp.concatenate([f[0] for f in fwd], axis=0)

        for step in range(n_tp):
            dy_rows = lax.dynamic_update_slice(dy_rows, dy_blocks[step], (offset(step), 0))
        dot = mm(wo, dy_rows, NT).astype(BF16)

        def exchange(arr_t):
            feats = arr_t.shape[0]
            split = arr_t.reshape(feats, n_tp, blk).transpose(1, 0, 2)
            return lax.all_to_all(split, "tp", 0, 0, tiled=True)

        def gathered_order(parts):
            feats, rows = parts.shape[1:]
            piece = feats // n_plane
            return parts.reshape(n_tp, n_plane, piece, rows).transpose(1, 0, 2, 3).reshape(n_tp * feats, rows)

        o_own = gathered_order(exchange(ot))
        y_blk = mm(o_own, wo_full, TN).astype(BF16)

        dq_parts, dk_parts, dv_parts, moved = [], [], [], []
        for h in range(kv_heads):
            with jax.named_scope(f"bwd_head_{h}"):
                dqt, dkv = attention_backward(rank_arr, qt, dot, fwd[h][0], fwd[h][1], kv_all, fwd[h][2],
                                              h, kv_heads, n_cp, groups, d, interpret)
            part = [dkv[:, j * n_rows:(j + 1) * n_rows] for j in range(n_cp)]
            if h < kv_heads - 1:
                dkv_own = part[0]
                for j in range(1, n_cp):
                    dkv_own = dkv_own + swap(part[j], "cp", j)
            else:
                near = swap(jnp.concatenate([part[1], part[3]], axis=1), "cp", 1)
                dkv_own = part[0] + near[:, :n_rows] + swap(part[2] + near[:, n_rows:], "cp", 2)
            dkv_own = dkv_own.astype(BF16)
            dq_parts.append(dqt)
            dk_parts.append(dkv_own[:d])
            dv_parts.append(dkv_own[d:])
            moved.append(exchange(jnp.concatenate([dqt, dkv_own], axis=0)))
        grads_own = gathered_order(jnp.concatenate(moved, axis=1))
        dx_blk = mm(grads_own, w_in_full, TN).astype(BF16)

        def weight_grad(parts):
            grad_t = mm(jnp.concatenate(parts, axis=0), x_rows).astype(BF16)
            return grad_t.reshape(-1, d, model).transpose(2, 0, 1)[None]

        grad_wo = mm(ot, dy_rows).astype(BF16).reshape(q_heads, d, model)
        return y_blk, dx_blk, weight_grad(dq_parts), weight_grad(dk_parts), weight_grad(dv_parts), grad_wo[None]

    return jax.shard_map(device_fn, mesh=mesh,
                         in_specs=(ROW_SPEC, HEAD_SPEC, HEAD_SPEC, HEAD_SPEC, OUT_W_SPEC, ROW_SPEC),
                         out_specs=(ROW_SPEC, ROW_SPEC, GRAD_SPEC, GRAD_SPEC, GRAD_SPEC, GRAD_OUT_SPEC),
                         check_vma=False)
```

```python
import functools

import jax
import jax.numpy as jnp
from jax import lax
from jax.experimental import pallas as pl
from jax.experimental.pallas import tpu as pltpu
from jax.sharding import PartitionSpec as P


ROW_SPEC = P(("dp", "cp", "tp"), None)
HEAD_SPEC = P(None, "tp", None)
OUT_W_SPEC = P("tp", None, None)
GRAD_SPEC = P(("dp", "cp"), None, "tp", None)
GRAD_OUT_SPEC = P(("dp", "cp"), "tp", None, None)
TN = (((0,), (0,)), ((), ()))
NT = (((1,), (1,)), ((), ()))
F32 = jnp.float32
BF16 = jnp.bfloat16


def mm(lhs, rhs, dims=(((1,), (0,)), ((), ()))):
    return lax.dot_general(lhs, rhs, dims, preferred_element_type=F32)


def chunk_offset(chunk, rank, n_shards, half):
    shard = jnp.where(chunk < n_shards, chunk, 2 * n_shards - 1 - chunk)
    upper = jnp.where(chunk < n_shards, 0, half)
    return pl.multiple_of(lax.bitwise_xor(shard, rank) * (2 * half) + upper, half)


def forward_kernel(n_shards, groups, d, half, h, kv_heads, rank_ref, qt_ref, kv_ref, ot_ref, lse_ref, kt_ref, q_pad, vt_s, m_s, l_s, acc_s):
    rank = rank_ref[0]
    kw = kv_heads * d
    sub = half // 2
    q_pad[...] = jnp.zeros_like(q_pad)
    for g in range(groups):
        q_pad[g, h * d:(h + 1) * d, :] = qt_ref[(h * groups + g) * d:(h * groups + g + 1) * d, :]

    def transpose_chunk(i, carry):
        rows = pl.ds(pl.multiple_of(i * half, half), half)
        kt_ref[:, rows] = kv_ref[rows, :kw].T[h * d:(h + 1) * d, :]
        vt_s[:, rows] = kv_ref[rows, kw:].T[h * d:(h + 1) * d, :]
        return carry

    lax.fori_loop(0, kv_ref.shape[0] // half, transpose_chunk, 0)

    def update(g, q_start, q_lo, q_len, k_off, k_len, masked):
        cols = slice(q_lo, q_lo + q_len)
        scores = mm(kv_ref[pl.ds(k_off, k_len), :kw], q_pad[g, :, q_start + q_lo:q_start + q_lo + q_len])
        if masked:
            k_id = lax.broadcasted_iota(jnp.int32, scores.shape, 0)
            q_id = lax.broadcasted_iota(jnp.int32, scores.shape, 1)
            scores = jnp.where(q_id >= k_id, scores, -jnp.inf)
        m_old = m_s[g:g + 1, cols]
        m_new = jnp.maximum(m_old, jnp.max(scores, axis=0, keepdims=True))
        prob = jnp.exp(scores - m_new)
        factor = jnp.exp(m_old - m_new)
        m_s[g:g + 1, cols] = m_new
        l_s[g:g + 1, cols] = l_s[g:g + 1, cols] * factor + jnp.sum(prob, axis=0, keepdims=True)
        pv = mm(vt_s[:, pl.ds(k_off, k_len)], prob.astype(BF16))
        acc_s[g * d:(g + 1) * d, cols] = acc_s[g * d:(g + 1) * d, cols] * factor + pv

    for q_half in range(2):
        q_start = q_half * half
        n_full = rank if q_half == 0 else 2 * n_shards - 1 - rank
        m_s[...] = jnp.full_like(m_s, -jnp.inf)
        l_s[...] = jnp.zeros_like(l_s)
        acc_s[...] = jnp.zeros_like(acc_s)
        off = chunk_offset(n_full, rank, n_shards, half)
        for g in range(groups):
            update(g, q_start, 0, half, off, sub, True)
        for g in range(groups):
            update(g, q_start, sub, sub, pl.multiple_of(off + sub, sub), sub, True)

        def full_block(chunk, carry):
            k_off = chunk_offset(chunk, rank, n_shards, half)
            for g in range(groups):
                update(g, q_start, 0, half, k_off, half, False)
            return carry

        lax.fori_loop(0, n_full, full_block, 0)
        for g in range(groups):
            l_row = l_s[g:g + 1, :]
            ot_ref[g * d:(g + 1) * d, q_start:q_start + half] = (acc_s[g * d:(g + 1) * d, :] / l_row).astype(BF16)
            lse_ref[g:g + 1, q_start:q_start + half] = m_s[g:g + 1, :] + jnp.log(l_row)


def backward_kernel(n_shards, groups, d, half, h, kv_heads, rank_ref, qt_ref, dot_ref, ot_ref, lse_ref, kv_ref, kt_ref,
                    dqt_ref, dkv_ref, q_pad, do_pad, delta_s, dq_s):
    rank = rank_ref[0]
    kw = kv_heads * d
    sub = half // 2
    q_pad[...] = jnp.zeros_like(q_pad)
    do_pad[...] = jnp.zeros_like(do_pad)
    for g in range(groups):
        rows = slice(g * d, (g + 1) * d)
        full = slice((h * groups + g) * d, (h * groups + g + 1) * d)
        q_pad[g, h * d:(h + 1) * d, :] = qt_ref[full, :]
        do_pad[g, h * d:(h + 1) * d, :] = dot_ref[full, :]
        delta_s[g:g + 1, :] = jnp.sum(dot_ref[full, :].astype(F32) * ot_ref[rows, :].astype(F32), axis=0, keepdims=True)
    dkv_ref[...] = jnp.zeros_like(dkv_ref)

    def update(q_start, q_lo, q_len, k_off, k_len, masked):
        lo = q_start + q_lo
        cols = slice(lo, lo + q_len)
        k_blk = kv_ref[pl.ds(k_off, k_len), :kw]
        v_blk = kv_ref[pl.ds(k_off, k_len), kw:]
        dk_sum, dv_sum = None, None
        for g in range(groups):
            rows = slice(g * d, (g + 1) * d)
            full = slice((h * groups + g) * d, (h * groups + g + 1) * d)
            scores = mm(k_blk, q_pad[g, :, cols])
            prob = jnp.exp(scores - lse_ref[g:g + 1, cols])
            if masked:
                k_id = lax.broadcasted_iota(jnp.int32, scores.shape, 0)
                q_id = lax.broadcasted_iota(jnp.int32, scores.shape, 1)
                prob = jnp.where(q_id >= k_id, prob, 0.0)
            d_prob = mm(v_blk, do_pad[g, :, cols])
            d_score = (prob * (d_prob - delta_s[g:g + 1, cols])).astype(BF16)
            dv = mm(dot_ref[full, cols], prob.astype(BF16), NT)
            dk = mm(qt_ref[full, cols], d_score, NT)
            dk_sum = dk if dk_sum is None else dk_sum + dk
            dv_sum = dv if dv_sum is None else dv_sum + dv
            dq_s[rows, q_lo:q_lo + q_len] += mm(kt_ref[:, pl.ds(k_off, k_len)], d_score)
        dkv_ref[:d, pl.ds(k_off, k_len)] += dk_sum
        dkv_ref[d:, pl.ds(k_off, k_len)] += dv_sum

    for q_half in range(2):
        q_start = q_half * half
        n_full = rank if q_half == 0 else 2 * n_shards - 1 - rank
        dq_s[...] = jnp.zeros_like(dq_s)
        off = chunk_offset(n_full, rank, n_shards, half)
        update(q_start, 0, half, off, sub, True)
        update(q_start, sub, sub, pl.multiple_of(off + sub, sub), sub, True)

        def full_block(chunk, carry):
            update(q_start, 0, half, chunk_offset(chunk, rank, n_shards, half), half, False)
            return carry

        lax.fori_loop(0, n_full, full_block, 0)
        dqt_ref[:, q_start:q_start + half] = (dq_s[...] * (d ** -0.5)).astype(BF16)


VMEM = pl.BlockSpec(memory_space=pltpu.VMEM)
SMEM = pl.BlockSpec(memory_space=pltpu.SMEM)


def attention_forward(rank_arr, qt, kv_all, h, kv_heads, n_shards, groups, d, interpret=False):
    n_rows = qt.shape[1]
    half = n_rows // 2
    kw = kv_all.shape[1] // 2
    pairs = groups * n_rows * n_rows * n_shards // 2
    return pl.pallas_call(
        functools.partial(forward_kernel, n_shards, groups, d, half, h, kv_heads),
        out_shape=(jax.ShapeDtypeStruct((groups * d, n_rows), BF16), jax.ShapeDtypeStruct((groups, n_rows), F32),
                   jax.ShapeDtypeStruct((d, kv_all.shape[0]), BF16)),
        in_specs=[SMEM, VMEM, VMEM],
        out_specs=(VMEM, VMEM, VMEM),
        scratch_shapes=[pltpu.VMEM((groups, kw, n_rows), BF16), pltpu.VMEM((d, kv_all.shape[0]), BF16),
                        pltpu.VMEM((groups, half), F32), pltpu.VMEM((groups, half), F32), pltpu.VMEM((groups * d, half), F32)],
        cost_estimate=pl.CostEstimate(flops=32 * d * pairs, bytes_accessed=6 << 20, transcendentals=pairs),
        compiler_params=pltpu.CompilerParams(vmem_limit_bytes=40 << 20),
        interpret=interpret,
    )(rank_arr, qt, kv_all)


def attention_backward(rank_arr, qt, dot, ot, lse, kv_all, kt, h, kv_heads, n_shards, groups, d, interpret=False):
    n_rows = qt.shape[1]
    half = n_rows // 2
    kw = kv_all.shape[1] // 2
    pairs = groups * n_rows * n_rows * n_shards // 2
    return pl.pallas_call(
        functools.partial(backward_kernel, n_shards, groups, d, half, h, kv_heads),
        out_shape=(jax.ShapeDtypeStruct((groups * d, n_rows), BF16), jax.ShapeDtypeStruct((2 * d, kv_all.shape[0]), F32)),
        in_specs=[SMEM] + [VMEM] * 6,
        out_specs=(VMEM, VMEM),
        scratch_shapes=[pltpu.VMEM((groups, kw, n_rows), BF16), pltpu.VMEM((groups, kw, n_rows), BF16),
                        pltpu.VMEM((groups, n_rows), F32), pltpu.VMEM((groups * d, half), F32)],
        cost_estimate=pl.CostEstimate(flops=40 * d * pairs, bytes_accessed=8 << 20, transcendentals=pairs),
        compiler_params=pltpu.CompilerParams(vmem_limit_bytes=40 << 20),
        interpret=interpret,
    )(rank_arr, qt, dot, ot, lse, kv_all, kt)


def solution(mesh, interpret=False):
    n_cp, n_tp, n_dp = mesh.shape["cp"], mesh.shape["tp"], mesh.shape["dp"]
    ring = [*range(0, n_tp, 2), *reversed(range(1, n_tp, 2))]
    hop = [(ring[i], ring[(i + 1) % n_tp]) for i in range(n_tp)]
    source = [[ring[(ring.index(z) - s) % n_tp] for z in range(n_tp)] for s in range(n_tp)]
    arrival = [[[source[s][z] for s in range(n_tp)].index(b) for z in range(n_tp)] for b in range(n_tp)]

    def swap(arr, axis, bit):
        return lax.ppermute(arr, axis, [(i, i ^ bit) for i in range(mesh.shape[axis])])

    def pick(table, idx):
        out = jnp.int32(table[0])
        for i, value in enumerate(table[1:], 1):
            out = jnp.where(idx == i, value, out)
        return out

    def device_fn(x_blk, w_query, w_key, w_value, w_out, dy_blk):
        rank = lax.axis_index("cp")
        z = lax.axis_index("tp")
        model, q_heads, d = w_query.shape
        kv_heads = w_key.shape[1]
        groups = q_heads // kv_heads
        gd = groups * d
        blk = x_blk.shape[0]
        n_rows = blk * n_tp
        rank_arr = rank.astype(jnp.int32).reshape(1)
        wqt = w_query.transpose(1, 2, 0).reshape(q_heads * d, model)
        wkt = w_key.transpose(1, 2, 0).reshape(kv_heads * d, model)
        wvt = w_value.transpose(1, 2, 0).reshape(kv_heads * d, model)
        wkvt = jnp.concatenate([wkt, wvt], axis=0)
        wo = w_out.reshape(q_heads * d, model)

        n_plane = n_dp * n_cp
        plane = lax.axis_index("dp") * n_cp + rank
        w_heads = jnp.concatenate([part for h in range(kv_heads) for part in
                                   (wqt[h * gd:(h + 1) * gd], wkt[h * d:(h + 1) * d], wvt[h * d:(h + 1) * d])], axis=0)
        n_in = w_heads.shape[0] // n_plane
        n_out = wo.shape[0] // n_plane
        w_in_piece = lax.dynamic_slice(w_heads, (plane * n_in, 0), (n_in, model))
        wo_piece = lax.dynamic_slice(wo, (plane * n_out, 0), (n_out, model))

        wo_line = lax.all_gather(wo_piece, "tp", axis=0, tiled=True)

        def offset(step):
            return pick(source[step], z) * blk

        x_rows = jnp.zeros((n_rows, model), BF16)
        qt = jnp.zeros((q_heads * d, n_rows), BF16)
        kv_blocks, kv_moved = [], []
        held = x_blk

        def cp_exchange(arr):
            near = swap(arr, "cp", 1)
            far = swap(arr, "cp", 2)
            return [arr, near, far, swap(far, "cp", 1)]

        for step in range(n_tp):
            following = lax.ppermute(held, "tp", hop) if step < n_tp - 1 else None
            if step == 1:
                wo_line, held = lax.optimization_barrier((wo_line, held))
                wo_full = lax.all_gather(wo_line, ("dp", "cp"), axis=0, tiled=True)
            if step == n_tp - 1:
                w_in_piece, held = lax.optimization_barrier((w_in_piece, held))
                w_in_line = lax.all_gather(w_in_piece, "tp", axis=0, tiled=True)
            kv_blocks.append(mm(held, wkvt, NT).astype(BF16))
            qt = lax.dynamic_update_slice(qt, mm(wqt, held, NT).astype(BF16) * BF16(d ** -0.5), (0, offset(step)))
            x_rows = lax.dynamic_update_slice(x_rows, held, (offset(step), 0))
            if step == n_tp - 2:
                kv_moved.append(cp_exchange(jnp.stack(kv_blocks)))
            if step == n_tp - 1:
                kv_moved.append(cp_exchange(kv_blocks[-1][None]))
            if following is not None:
                following, qt, x_rows, kv_blocks[-1], kv_moved = lax.optimization_barrier(
                    (following, qt, x_rows, kv_blocks[-1], kv_moved))
                held = following
        dy_first, _ = lax.optimization_barrier((dy_blk, held))
        slots = []
        for slot in range(n_cp):
            by_arrival = jnp.concatenate([kv_moved[0][slot], kv_moved[1][slot]], axis=0)
            slots += [lax.dynamic_index_in_dim(by_arrival, pick(arrival[b], z), 0, keepdims=False) for b in range(n_tp)]
        kv_all = jnp.concatenate(slots, axis=0)

        dy_rows = jnp.zeros((n_rows, model), BF16)
        dot = jnp.zeros((q_heads * d, n_rows), BF16)
        dy_held = dy_first
        fwd = []
        for step in range(n_tp):
            following = lax.ppermute(dy_held, "tp", hop) if step < n_tp - 1 else None
            dy_rows = lax.dynamic_update_slice(dy_rows, dy_held, (offset(step), 0))
            dot = lax.dynamic_update_slice(dot, mm(wo, dy_held, NT).astype(BF16), (0, offset(step)))
            if 1 <= step <= kv_heads:
                h = step - 1
                qt, kv_all, x_rows, dy_rows, dot = lax.optimization_barrier((qt, kv_all, x_rows, dy_rows, dot))
                fwd.append(attention_forward(rank_arr, qt, kv_all, h, kv_heads, n_cp, groups, d, interpret))
                if h == 0:
                    ot_0, w_in_line = lax.optimization_barrier((fwd[0][0], w_in_line))
                    fwd[0] = (ot_0,) + tuple(fwd[0][1:])
                    w_in_full = lax.all_gather(w_in_line, ("dp", "cp"), axis=0, tiled=True)
                if following is not None:
                    following, ot_h = lax.optimization_barrier((following, fwd[h][0]))
                    fwd[h] = (ot_h,) + tuple(fwd[h][1:])
            dy_held = following
        ot = jnp.concatenate([f[0] for f in fwd], axis=0)

        def exchange(arr_t):
            sent = [lax.dynamic_slice(arr_t, (0, lax.bitwise_xor(z, k) * blk), (arr_t.shape[0], blk)) for k in range(n_tp)]
            return [sent[0]] + [swap(sent[k], "tp", k) for k in range(1, n_tp)]

        def gathered_order(parts):
            stacked = jnp.stack(parts)
            feats, rows = stacked.shape[1:]
            by_z = jnp.stack([lax.dynamic_index_in_dim(stacked, lax.bitwise_xor(z, t), 0, keepdims=False) for t in range(n_tp)])
            return by_z.reshape(n_tp, n_plane, feats // n_plane, rows).transpose(1, 0, 2, 3).reshape(n_tp * feats, rows)

        o_parts = exchange(ot)
        o_own = gathered_order(o_parts)
        y_blk = mm(o_own, wo_full, TN).astype(BF16)

        dq_parts, dkv_parts, moved, waiting = [], [], [], None
        for h in range(kv_heads):
            dqt, dkv = attention_backward(rank_arr, qt, dot, fwd[h][0], fwd[h][1], kv_all, fwd[h][2],
                                          h, kv_heads, n_cp, groups, d, interpret)
            dq_parts.append(dqt)
            part = [dkv[:, j * n_rows:(j + 1) * n_rows] for j in range(n_cp)]
            if h < kv_heads - 1:
                moved.append(exchange(dqt))
                far_parts = [swap(part[j], "cp", j) for j in range(1, n_cp)]
                waiting = (part[0], far_parts)
            else:
                near = swap(jnp.concatenate([part[1], part[3]], axis=1), "cp", 1)
                if waiting is not None:
                    own, far_parts = waiting
                    dkv_own = functools.reduce(jnp.add, far_parts, own).astype(BF16)
                    dkv_parts.append(dkv_own)
                    moved.append(exchange(jnp.concatenate([dkv_own, dqt], axis=0)))
                else:
                    moved.append(exchange(dqt))
                dkv_own = (part[0] + near[:, :n_rows] + swap(part[2] + near[:, n_rows:], "cp", 2)).astype(BF16)
                dkv_parts.append(dkv_own)
                moved.append(exchange(dkv_own))
        grads_own = gathered_order([jnp.concatenate([m[k] for m in moved], axis=0) for k in range(n_tp)])
        dx_blk = mm(grads_own, w_in_full, TN).astype(BF16)

        def weight_layout(grad_t):
            return grad_t.reshape(-1, d, model).transpose(2, 0, 1)[None]

        dk_dv = jnp.concatenate([part[:d] for part in dkv_parts] + [part[d:] for part in dkv_parts], axis=0)
        grad_wq = mm(jnp.concatenate(dq_parts, axis=0), x_rows).astype(BF16)
        grad_wkv = mm(dk_dv, x_rows).astype(BF16)
        grad_wo = mm(ot, dy_rows).astype(BF16).reshape(q_heads, d, model)
        return (y_blk, dx_blk, weight_layout(grad_wq), weight_layout(grad_wkv[:kv_heads * d]), weight_layout(grad_wkv[kv_heads * d:]),
                grad_wo[None])

    return jax.shard_map(device_fn, mesh=mesh,
                         in_specs=(ROW_SPEC, HEAD_SPEC, HEAD_SPEC, HEAD_SPEC, OUT_W_SPEC, ROW_SPEC),
                         out_specs=(ROW_SPEC, ROW_SPEC, GRAD_SPEC, GRAD_SPEC, GRAD_SPEC, GRAD_OUT_SPEC),
                         check_vma=False)
```

```python
import functools

import jax
import jax.numpy as jnp
from jax import lax
from jax.experimental import pallas as pl
from jax.experimental.pallas import tpu as pltpu
from jax.sharding import PartitionSpec as P


ROW_SPEC = P(("dp", "cp", "tp"), None)
HEAD_SPEC = P(None, "tp", None)
OUT_W_SPEC = P("tp", None, None)
GRAD_SPEC = P(("dp", "cp"), None, "tp", None)
GRAD_OUT_SPEC = P(("dp", "cp"), "tp", None, None)
TN = (((0,), (0,)), ((), ()))
NT = (((1,), (1,)), ((), ()))
F32 = jnp.float32
BF16 = jnp.bfloat16


def mm(lhs, rhs, dims=(((1,), (0,)), ((), ()))):
    return lax.dot_general(lhs, rhs, dims, preferred_element_type=F32)


def chunk_offset(chunk, rank, n_shards, half):
    shard = jnp.where(chunk < n_shards, chunk, 2 * n_shards - 1 - chunk)
    upper = jnp.where(chunk < n_shards, 0, half)
    return pl.multiple_of(lax.bitwise_xor(shard, rank) * (2 * half) + upper, half)


def forward_kernel(n_shards, groups, d, half, h, kv_heads, rank_ref, qt_ref, kv_ref, ot_ref, lse_ref, kt_ref, q_pad, vt_s, m_s, l_s, acc_s):
    rank = rank_ref[0]
    kw = kv_heads * d
    sub = half // 2
    q_pad[...] = jnp.zeros_like(q_pad)
    for g in range(groups):
        q_pad[g, h * d:(h + 1) * d, :] = qt_ref[(h * groups + g) * d:(h * groups + g + 1) * d, :]

    def transpose_chunk(i, carry):
        rows = pl.ds(pl.multiple_of(i * half, half), half)
        kt_ref[:, rows] = kv_ref[rows, :kw].T[h * d:(h + 1) * d, :]
        vt_s[:, rows] = kv_ref[rows, kw:].T[h * d:(h + 1) * d, :]
        return carry

    lax.fori_loop(0, kv_ref.shape[0] // half, transpose_chunk, 0)

    def update(g, q_start, q_lo, q_len, k_off, k_len, masked):
        cols = slice(q_lo, q_lo + q_len)
        scores = mm(kv_ref[pl.ds(k_off, k_len), :kw], q_pad[g, :, q_start + q_lo:q_start + q_lo + q_len])
        if masked:
            k_id = lax.broadcasted_iota(jnp.int32, scores.shape, 0)
            q_id = lax.broadcasted_iota(jnp.int32, scores.shape, 1)
            scores = jnp.where(q_id >= k_id, scores, -jnp.inf)
        m_old = m_s[g:g + 1, cols]
        m_new = jnp.maximum(m_old, jnp.max(scores, axis=0, keepdims=True))
        prob = jnp.exp(scores - m_new)
        factor = jnp.exp(m_old - m_new)
        m_s[g:g + 1, cols] = m_new
        l_s[g:g + 1, cols] = l_s[g:g + 1, cols] * factor + jnp.sum(prob, axis=0, keepdims=True)
        pv = mm(vt_s[:, pl.ds(k_off, k_len)], prob.astype(BF16))
        acc_s[g * d:(g + 1) * d, cols] = acc_s[g * d:(g + 1) * d, cols] * factor + pv

    for q_half in range(2):
        q_start = q_half * half
        n_full = rank if q_half == 0 else 2 * n_shards - 1 - rank
        m_s[...] = jnp.full_like(m_s, -jnp.inf)
        l_s[...] = jnp.zeros_like(l_s)
        acc_s[...] = jnp.zeros_like(acc_s)
        off = chunk_offset(n_full, rank, n_shards, half)
        for g in range(groups):
            update(g, q_start, 0, half, off, sub, True)
        for g in range(groups):
            update(g, q_start, sub, sub, pl.multiple_of(off + sub, sub), sub, True)

        def full_block(chunk, carry):
            k_off = chunk_offset(chunk, rank, n_shards, half)
            for g in range(groups):
                update(g, q_start, 0, half, k_off, half, False)
            return carry

        lax.fori_loop(0, n_full, full_block, 0)
        for g in range(groups):
            l_row = l_s[g:g + 1, :]
            ot_ref[g * d:(g + 1) * d, q_start:q_start + half] = (acc_s[g * d:(g + 1) * d, :] / l_row).astype(BF16)
            lse_ref[g:g + 1, q_start:q_start + half] = m_s[g:g + 1, :] + jnp.log(l_row)


def backward_kernel(n_shards, groups, d, half, h, kv_heads, rank_ref, qt_ref, dot_ref, ot_ref, lse_ref, kv_ref, kt_ref,
                    dqt_ref, dkv_ref, q_pad, do_pad, delta_s, dq_s):
    rank = rank_ref[0]
    kw = kv_heads * d
    sub = half // 2
    q_pad[...] = jnp.zeros_like(q_pad)
    do_pad[...] = jnp.zeros_like(do_pad)
    for g in range(groups):
        rows = slice(g * d, (g + 1) * d)
        full = slice((h * groups + g) * d, (h * groups + g + 1) * d)
        q_pad[g, h * d:(h + 1) * d, :] = qt_ref[full, :]
        do_pad[g, h * d:(h + 1) * d, :] = dot_ref[full, :]
        delta_s[g:g + 1, :] = jnp.sum(dot_ref[full, :].astype(F32) * ot_ref[rows, :].astype(F32), axis=0, keepdims=True)
    dkv_ref[...] = jnp.zeros_like(dkv_ref)

    def update(q_start, q_lo, q_len, k_off, k_len, masked):
        lo = q_start + q_lo
        cols = slice(lo, lo + q_len)
        k_blk = kv_ref[pl.ds(k_off, k_len), :kw]
        v_blk = kv_ref[pl.ds(k_off, k_len), kw:]
        dk_sum, dv_sum = None, None
        for g in range(groups):
            rows = slice(g * d, (g + 1) * d)
            full = slice((h * groups + g) * d, (h * groups + g + 1) * d)
            scores = mm(k_blk, q_pad[g, :, cols])
            prob = jnp.exp(scores - lse_ref[g:g + 1, cols])
            if masked:
                k_id = lax.broadcasted_iota(jnp.int32, scores.shape, 0)
                q_id = lax.broadcasted_iota(jnp.int32, scores.shape, 1)
                prob = jnp.where(q_id >= k_id, prob, 0.0)
            d_prob = mm(v_blk, do_pad[g, :, cols])
            d_score = (prob * (d_prob - delta_s[g:g + 1, cols])).astype(BF16)
            dv = mm(dot_ref[full, cols], prob.astype(BF16), NT)
            dk = mm(qt_ref[full, cols], d_score, NT)
            dk_sum = dk if dk_sum is None else dk_sum + dk
            dv_sum = dv if dv_sum is None else dv_sum + dv
            dq_s[rows, q_lo:q_lo + q_len] += mm(kt_ref[:, pl.ds(k_off, k_len)], d_score)
        dkv_ref[:d, pl.ds(k_off, k_len)] += dk_sum
        dkv_ref[d:, pl.ds(k_off, k_len)] += dv_sum

    for q_half in range(2):
        q_start = q_half * half
        n_full = rank if q_half == 0 else 2 * n_shards - 1 - rank
        dq_s[...] = jnp.zeros_like(dq_s)
        off = chunk_offset(n_full, rank, n_shards, half)
        update(q_start, 0, half, off, sub, True)
        update(q_start, sub, sub, pl.multiple_of(off + sub, sub), sub, True)

        def full_block(chunk, carry):
            update(q_start, 0, half, chunk_offset(chunk, rank, n_shards, half), half, False)
            return carry

        lax.fori_loop(0, n_full, full_block, 0)
        dqt_ref[:, q_start:q_start + half] = (dq_s[...] * (d ** -0.5)).astype(BF16)


VMEM = pl.BlockSpec(memory_space=pltpu.VMEM)
SMEM = pl.BlockSpec(memory_space=pltpu.SMEM)


def attention_forward(rank_arr, qt, kv_all, h, kv_heads, n_shards, groups, d, interpret=False):
    n_rows = qt.shape[1]
    half = n_rows // 2
    kw = kv_all.shape[1] // 2
    pairs = groups * n_rows * n_rows * n_shards // 2
    return pl.pallas_call(
        functools.partial(forward_kernel, n_shards, groups, d, half, h, kv_heads),
        out_shape=(jax.ShapeDtypeStruct((groups * d, n_rows), BF16), jax.ShapeDtypeStruct((groups, n_rows), F32),
                   jax.ShapeDtypeStruct((d, kv_all.shape[0]), BF16)),
        in_specs=[SMEM, VMEM, VMEM],
        out_specs=(VMEM, VMEM, VMEM),
        scratch_shapes=[pltpu.VMEM((groups, kw, n_rows), BF16), pltpu.VMEM((d, kv_all.shape[0]), BF16),
                        pltpu.VMEM((groups, half), F32), pltpu.VMEM((groups, half), F32), pltpu.VMEM((groups * d, half), F32)],
        cost_estimate=pl.CostEstimate(flops=32 * d * pairs, bytes_accessed=6 << 20, transcendentals=pairs),
        compiler_params=pltpu.CompilerParams(vmem_limit_bytes=40 << 20),
        interpret=interpret,
    )(rank_arr, qt, kv_all)


def attention_backward(rank_arr, qt, dot, ot, lse, kv_all, kt, h, kv_heads, n_shards, groups, d, interpret=False):
    n_rows = qt.shape[1]
    half = n_rows // 2
    kw = kv_all.shape[1] // 2
    pairs = groups * n_rows * n_rows * n_shards // 2
    return pl.pallas_call(
        functools.partial(backward_kernel, n_shards, groups, d, half, h, kv_heads),
        out_shape=(jax.ShapeDtypeStruct((groups * d, n_rows), BF16), jax.ShapeDtypeStruct((2 * d, kv_all.shape[0]), F32)),
        in_specs=[SMEM] + [VMEM] * 6,
        out_specs=(VMEM, VMEM),
        scratch_shapes=[pltpu.VMEM((groups, kw, n_rows), BF16), pltpu.VMEM((groups, kw, n_rows), BF16),
                        pltpu.VMEM((groups, n_rows), F32), pltpu.VMEM((groups * d, half), F32)],
        cost_estimate=pl.CostEstimate(flops=40 * d * pairs, bytes_accessed=8 << 20, transcendentals=pairs),
        compiler_params=pltpu.CompilerParams(vmem_limit_bytes=40 << 20),
        interpret=interpret,
    )(rank_arr, qt, dot, ot, lse, kv_all, kt)


def assemble_kernel(n_rows, source_ref, *refs):
    out_ref = refs[-1]
    n_slots = (len(refs) - 1) // 2
    for slot in range(n_slots):
        arrived = 0
        for ref in (refs[2 * slot], refs[2 * slot + 1]):
            for i in range(ref.shape[0]):
                blk = ref.shape[1]
                start = pl.multiple_of(slot * n_rows + source_ref[arrived] * blk, blk)
                out_ref[pl.ds(start, blk), :] = ref[i]
                arrived += 1


def assemble_kv(source_arr, pieces, n_rows, interpret=False):
    n_slots = len(pieces) // 2
    width = pieces[0].shape[2]
    return pl.pallas_call(
        functools.partial(assemble_kernel, n_rows),
        out_shape=jax.ShapeDtypeStruct((n_slots * n_rows, width), BF16),
        in_specs=[SMEM] + [VMEM] * len(pieces),
        out_specs=VMEM,
        cost_estimate=pl.CostEstimate(flops=1 << 20, bytes_accessed=4 * n_slots * n_rows * width, transcendentals=0),
        compiler_params=pltpu.CompilerParams(vmem_limit_bytes=16 << 20),
        name="assemble_kv",
        interpret=interpret,
    )(source_arr, *pieces)


def solution(mesh, interpret=False):
    n_cp, n_tp, n_dp = mesh.shape["cp"], mesh.shape["tp"], mesh.shape["dp"]
    ring = [*range(0, n_tp, 2), *reversed(range(1, n_tp, 2))]
    hop = [(ring[i], ring[(i + 1) % n_tp]) for i in range(n_tp)]
    source = [[ring[(ring.index(z) - s) % n_tp] for z in range(n_tp)] for s in range(n_tp)]

    def swap(arr, axis, bit):
        return lax.ppermute(arr, axis, [(i, i ^ bit) for i in range(mesh.shape[axis])])

    def pick(table, idx):
        out = jnp.int32(table[0])
        for i, value in enumerate(table[1:], 1):
            out = jnp.where(idx == i, value, out)
        return out

    def device_fn(x_blk, w_query, w_key, w_value, w_out, dy_blk):
        rank = lax.axis_index("cp")
        z = lax.axis_index("tp")
        model, q_heads, d = w_query.shape
        kv_heads = w_key.shape[1]
        groups = q_heads // kv_heads
        gd = groups * d
        blk = x_blk.shape[0]
        n_rows = blk * n_tp
        rank_arr = rank.astype(jnp.int32).reshape(1)
        wqt = w_query.transpose(1, 2, 0).reshape(q_heads * d, model)
        wkt = w_key.transpose(1, 2, 0).reshape(kv_heads * d, model)
        wvt = w_value.transpose(1, 2, 0).reshape(kv_heads * d, model)
        wkvt = jnp.concatenate([wkt, wvt], axis=0)
        wo = w_out.reshape(q_heads * d, model)

        n_plane = n_dp * n_cp
        plane = lax.axis_index("dp") * n_cp + rank
        w_heads = jnp.concatenate([part for h in range(kv_heads) for part in
                                   (wqt[h * gd:(h + 1) * gd], wkt[h * d:(h + 1) * d], wvt[h * d:(h + 1) * d])], axis=0)
        n_in = w_heads.shape[0] // n_plane
        n_out = wo.shape[0] // n_plane
        w_in_piece = lax.dynamic_slice(w_heads, (plane * n_in, 0), (n_in, model))
        wo_piece = lax.dynamic_slice(wo, (plane * n_out, 0), (n_out, model))

        wo_line = lax.all_gather(wo_piece, "tp", axis=0, tiled=True)

        def offset(step):
            return pick(source[step], z) * blk

        x_rows = jnp.zeros((n_rows, model), BF16)
        qt = jnp.zeros((q_heads * d, n_rows), BF16)
        kv_blocks, kv_moved = [], []
        held = x_blk

        def cp_exchange(arr):
            near = swap(arr, "cp", 1)
            far = swap(arr, "cp", 2)
            return [arr, near, far, swap(far, "cp", 1)]

        for step in range(n_tp):
            following = lax.ppermute(held, "tp", hop) if step < n_tp - 1 else None
            if step == 1:
                wo_line, held = lax.optimization_barrier((wo_line, held))
                wo_full = lax.all_gather(wo_line, ("dp", "cp"), axis=0, tiled=True)
            kv_blocks.append(mm(held, wkvt, NT).astype(BF16))
            qt = lax.dynamic_update_slice(qt, mm(wqt, held, NT).astype(BF16) * BF16(d ** -0.5), (0, offset(step)))
            x_rows = lax.dynamic_update_slice(x_rows, held, (offset(step), 0))
            if step == n_tp - 2:
                kv_moved.append(cp_exchange(jnp.stack(kv_blocks)))
            if step == n_tp - 1:
                kv_moved.append(cp_exchange(kv_blocks[-1][None]))
            if following is not None:
                following, qt, x_rows, kv_blocks[-1], kv_moved = lax.optimization_barrier(
                    (following, qt, x_rows, kv_blocks[-1], kv_moved))
                held = following
        dy_first, _ = lax.optimization_barrier((dy_blk, held))
        source_arr = jnp.stack([pick(source[step], z) for step in range(n_tp)])
        pieces = [kv_moved[i][slot] for slot in range(n_cp) for i in range(2)]
        kv_all = assemble_kv(source_arr, pieces, n_rows, interpret)

        dy_rows = jnp.zeros((n_rows, model), BF16)
        dot = jnp.zeros((q_heads * d, n_rows), BF16)
        dy_held = dy_first
        fwd = []
        for step in range(n_tp):
            following = lax.ppermute(dy_held, "tp", hop) if step < n_tp - 1 else None
            dy_rows = lax.dynamic_update_slice(dy_rows, dy_held, (offset(step), 0))
            dot = lax.dynamic_update_slice(dot, mm(wo, dy_held, NT).astype(BF16), (0, offset(step)))
            if 1 <= step <= kv_heads:
                h = step - 1
                qt, kv_all, x_rows, dy_rows, dot = lax.optimization_barrier((qt, kv_all, x_rows, dy_rows, dot))
                fwd.append(attention_forward(rank_arr, qt, kv_all, h, kv_heads, n_cp, groups, d, interpret))
                if following is not None:
                    following, ot_h = lax.optimization_barrier((following, fwd[h][0]))
                    fwd[h] = (ot_h,) + tuple(fwd[h][1:])
            dy_last, dy_held = dy_held, following
        ot = jnp.concatenate([f[0] for f in fwd], axis=0)
        w_in_piece, wo_full, dy_held = lax.optimization_barrier((w_in_piece, wo_full, dy_last))
        w_in_line = lax.all_gather(w_in_piece, "tp", axis=0, tiled=True)

        def exchange(arr_t):
            sent = [lax.dynamic_slice(arr_t, (0, lax.bitwise_xor(z, k) * blk), (arr_t.shape[0], blk)) for k in range(n_tp)]
            return [sent[0]] + [swap(sent[k], "tp", k) for k in range(1, n_tp)]

        def gathered_order(parts, n_pieces):
            stacked = jnp.stack(parts)
            feats, rows = stacked.shape[1:]
            by_z = jnp.stack([lax.dynamic_index_in_dim(stacked, lax.bitwise_xor(z, t), 0, keepdims=False) for t in range(n_tp)])
            return by_z.reshape(n_tp, n_pieces, feats // n_pieces, rows).transpose(1, 0, 2, 3).reshape(n_tp * feats, rows)

        o_parts = exchange(ot)
        o_own = gathered_order(o_parts, n_plane)
        y_blk = mm(o_own, wo_full, TN).astype(BF16)

        dq_parts, dkv_parts, moved, waiting = [], [], [], None
        for h in range(kv_heads):
            dqt, dkv = attention_backward(rank_arr, qt, dot, fwd[h][0], fwd[h][1], kv_all, fwd[h][2],
                                          h, kv_heads, n_cp, groups, d, interpret)
            dq_parts.append(dqt)
            part = [dkv[:, j * n_rows:(j + 1) * n_rows] for j in range(n_cp)]
            if h < kv_heads - 1:
                moved.append(exchange(dqt))
                far_parts = [swap(part[j], "cp", j) for j in range(1, n_cp)]
                waiting = (part[0], far_parts)
                if h == 0:
                    w_in_line, qt = lax.optimization_barrier((w_in_line, lax.optimization_barrier((qt, dqt))[0]))
                    w_in_full = lax.all_gather(w_in_line, ("dp", "cp"), axis=0, tiled=True)
            else:
                near = swap(jnp.concatenate([part[1], part[3]], axis=1), "cp", 1)
                if waiting is not None:
                    own, far_parts = waiting
                    dkv_own = functools.reduce(jnp.add, far_parts, own).astype(BF16)
                    dkv_parts.append(dkv_own)
                    moved.append(exchange(jnp.concatenate([dkv_own, dqt], axis=0)))
                else:
                    moved.append(exchange(dqt))
                far = swap(part[2] + near[:, n_rows:], "cp", 2)
                far, y_blk = lax.optimization_barrier((far, y_blk))
                dkv_own = (part[0] + near[:, :n_rows] + far).astype(BF16)
                dkv_parts.append(dkv_own)
                moved.append(exchange(dkv_own))
        n_early = (n_in * n_plane - dkv_parts[-1].shape[0]) // n_in
        early = [jnp.concatenate([m[k] for m in moved[:-1]], axis=0) for k in range(n_tp)]
        split = n_early * n_in * n_tp
        dx_early = mm(gathered_order([part[:n_early * n_in] for part in early], n_early), w_in_full[:split], TN)
        dx_early, last = lax.optimization_barrier((dx_early, moved[-1]))
        late = [jnp.concatenate([early[k][n_early * n_in:], last[k]], axis=0) for k in range(n_tp)]
        dx_blk = (dx_early + mm(gathered_order(late, n_plane - n_early), w_in_full[split:], TN)).astype(BF16)

        def weight_layout(grad_t):
            return grad_t.reshape(-1, d, model).transpose(2, 0, 1)[None]

        dk_dv = jnp.concatenate([part[:d] for part in dkv_parts] + [part[d:] for part in dkv_parts], axis=0)
        grad_wq = mm(jnp.concatenate(dq_parts, axis=0), x_rows).astype(BF16)
        grad_wkv = mm(dk_dv, x_rows).astype(BF16)
        grad_wo = mm(ot, dy_rows).astype(BF16).reshape(q_heads, d, model)
        return (y_blk, dx_blk, weight_layout(grad_wq), weight_layout(grad_wkv[:kv_heads * d]), weight_layout(grad_wkv[kv_heads * d:]),
                grad_wo[None])

    return jax.shard_map(device_fn, mesh=mesh,
                         in_specs=(ROW_SPEC, HEAD_SPEC, HEAD_SPEC, HEAD_SPEC, OUT_W_SPEC, ROW_SPEC),
                         out_specs=(ROW_SPEC, ROW_SPEC, GRAD_SPEC, GRAD_SPEC, GRAD_SPEC, GRAD_OUT_SPEC),
                         check_vma=False)
```

```python
import functools

import jax
import jax.numpy as jnp
from jax import lax
from jax.experimental import pallas as pl
from jax.experimental.pallas import tpu as pltpu
from jax.sharding import PartitionSpec as P


ROW_SPEC = P(("dp", "cp", "tp"), None)
HEAD_SPEC = P(None, "tp", None)
OUT_W_SPEC = P("tp", None, None)
GRAD_SPEC = P(("dp", "cp"), None, "tp", None)
GRAD_OUT_SPEC = P(("dp", "cp"), "tp", None, None)
TN = (((0,), (0,)), ((), ()))
NT = (((1,), (1,)), ((), ()))
F32 = jnp.float32
BF16 = jnp.bfloat16


def mm(lhs, rhs, dims=(((1,), (0,)), ((), ()))):
    return lax.dot_general(lhs, rhs, dims, preferred_element_type=F32)


def chunk_offset(chunk, rank, n_shards, half):
    shard = jnp.where(chunk < n_shards, chunk, 2 * n_shards - 1 - chunk)
    upper = jnp.where(chunk < n_shards, 0, half)
    return pl.multiple_of(lax.bitwise_xor(shard, rank) * (2 * half) + upper, half)


def forward_kernel(n_shards, groups, d, half, h, kv_heads, rank_ref, qt_ref, kv_ref, ot_ref, lse_ref, kt_ref, q_pad, vt_s, m_s, l_s, acc_s):
    rank = rank_ref[0]
    kw = kv_heads * d
    sub = half // 2
    q_pad[...] = jnp.zeros_like(q_pad)
    for g in range(groups):
        q_pad[g, h * d:(h + 1) * d, :] = qt_ref[(h * groups + g) * d:(h * groups + g + 1) * d, :]

    def transpose_chunk(i, carry):
        rows = pl.ds(pl.multiple_of(i * half, half), half)
        kt_ref[:, rows] = kv_ref[rows, :kw].T[h * d:(h + 1) * d, :]
        vt_s[:, rows] = kv_ref[rows, kw:].T[h * d:(h + 1) * d, :]
        return carry

    lax.fori_loop(0, kv_ref.shape[0] // half, transpose_chunk, 0)

    def update(g, q_start, q_lo, q_len, k_off, k_len, masked):
        cols = slice(q_lo, q_lo + q_len)
        scores = mm(kv_ref[pl.ds(k_off, k_len), :kw], q_pad[g, :, q_start + q_lo:q_start + q_lo + q_len])
        if masked:
            k_id = lax.broadcasted_iota(jnp.int32, scores.shape, 0)
            q_id = lax.broadcasted_iota(jnp.int32, scores.shape, 1)
            scores = jnp.where(q_id >= k_id, scores, -jnp.inf)
        m_old = m_s[g:g + 1, cols]
        m_new = jnp.maximum(m_old, jnp.max(scores, axis=0, keepdims=True))
        prob = jnp.exp(scores - m_new)
        factor = jnp.exp(m_old - m_new)
        m_s[g:g + 1, cols] = m_new
        l_s[g:g + 1, cols] = l_s[g:g + 1, cols] * factor + jnp.sum(prob, axis=0, keepdims=True)
        pv = mm(vt_s[:, pl.ds(k_off, k_len)], prob.astype(BF16))
        acc_s[g * d:(g + 1) * d, cols] = acc_s[g * d:(g + 1) * d, cols] * factor + pv

    for q_half in range(2):
        q_start = q_half * half
        n_full = rank if q_half == 0 else 2 * n_shards - 1 - rank
        m_s[...] = jnp.full_like(m_s, -jnp.inf)
        l_s[...] = jnp.zeros_like(l_s)
        acc_s[...] = jnp.zeros_like(acc_s)
        off = chunk_offset(n_full, rank, n_shards, half)
        for g in range(groups):
            update(g, q_start, 0, half, off, sub, True)
        for g in range(groups):
            update(g, q_start, sub, sub, pl.multiple_of(off + sub, sub), sub, True)

        def full_block(chunk, carry):
            k_off = chunk_offset(chunk, rank, n_shards, half)
            for g in range(groups):
                update(g, q_start, 0, half, k_off, half, False)
            return carry

        lax.fori_loop(0, n_full, full_block, 0)
        for g in range(groups):
            l_row = l_s[g:g + 1, :]
            ot_ref[g * d:(g + 1) * d, q_start:q_start + half] = (acc_s[g * d:(g + 1) * d, :] / l_row).astype(BF16)
            lse_ref[g:g + 1, q_start:q_start + half] = m_s[g:g + 1, :] + jnp.log(l_row)


def backward_kernel(n_shards, groups, d, half, h, kv_heads, rank_ref, qt_ref, dot_ref, ot_ref, lse_ref, kv_ref, kt_ref,
                    dqt_ref, dkv_ref, q_pad, do_pad, delta_s, dq_s):
    rank = rank_ref[0]
    kw = kv_heads * d
    sub = half // 2
    q_pad[...] = jnp.zeros_like(q_pad)
    do_pad[...] = jnp.zeros_like(do_pad)
    for g in range(groups):
        rows = slice(g * d, (g + 1) * d)
        full = slice((h * groups + g) * d, (h * groups + g + 1) * d)
        q_pad[g, h * d:(h + 1) * d, :] = qt_ref[full, :]
        do_pad[g, h * d:(h + 1) * d, :] = dot_ref[full, :]
        delta_s[g:g + 1, :] = jnp.sum(dot_ref[full, :].astype(F32) * ot_ref[rows, :].astype(F32), axis=0, keepdims=True)
    dkv_ref[...] = jnp.zeros_like(dkv_ref)

    def update(q_start, q_lo, q_len, k_off, k_len, masked):
        lo = q_start + q_lo
        cols = slice(lo, lo + q_len)
        k_blk = kv_ref[pl.ds(k_off, k_len), :kw]
        v_blk = kv_ref[pl.ds(k_off, k_len), kw:]
        dk_sum, dv_sum = None, None
        for g in range(groups):
            rows = slice(g * d, (g + 1) * d)
            full = slice((h * groups + g) * d, (h * groups + g + 1) * d)
            scores = mm(k_blk, q_pad[g, :, cols])
            prob = jnp.exp(scores - lse_ref[g:g + 1, cols])
            if masked:
                k_id = lax.broadcasted_iota(jnp.int32, scores.shape, 0)
                q_id = lax.broadcasted_iota(jnp.int32, scores.shape, 1)
                prob = jnp.where(q_id >= k_id, prob, 0.0)
            d_prob = mm(v_blk, do_pad[g, :, cols])
            d_score = (prob * (d_prob - delta_s[g:g + 1, cols])).astype(BF16)
            dv = mm(dot_ref[full, cols], prob.astype(BF16), NT)
            dk = mm(qt_ref[full, cols], d_score, NT)
            dk_sum = dk if dk_sum is None else dk_sum + dk
            dv_sum = dv if dv_sum is None else dv_sum + dv
            dq_s[rows, q_lo:q_lo + q_len] += mm(kt_ref[:, pl.ds(k_off, k_len)], d_score)
        dkv_ref[:d, pl.ds(k_off, k_len)] += dk_sum
        dkv_ref[d:, pl.ds(k_off, k_len)] += dv_sum

    for q_half in range(2):
        q_start = q_half * half
        n_full = rank if q_half == 0 else 2 * n_shards - 1 - rank
        dq_s[...] = jnp.zeros_like(dq_s)
        off = chunk_offset(n_full, rank, n_shards, half)
        update(q_start, 0, half, off, sub, True)
        update(q_start, sub, sub, pl.multiple_of(off + sub, sub), sub, True)

        def full_block(chunk, carry):
            update(q_start, 0, half, chunk_offset(chunk, rank, n_shards, half), half, False)
            return carry

        lax.fori_loop(0, n_full, full_block, 0)
        dqt_ref[:, q_start:q_start + half] = (dq_s[...] * (d ** -0.5)).astype(BF16)


VMEM = pl.BlockSpec(memory_space=pltpu.VMEM)
SMEM = pl.BlockSpec(memory_space=pltpu.SMEM)


def attention_forward(rank_arr, qt, kv_all, h, kv_heads, n_shards, groups, d, interpret=False):
    n_rows = qt.shape[1]
    half = n_rows // 2
    kw = kv_all.shape[1] // 2
    pairs = groups * n_rows * n_rows * n_shards // 2
    return pl.pallas_call(
        functools.partial(forward_kernel, n_shards, groups, d, half, h, kv_heads),
        out_shape=(jax.ShapeDtypeStruct((groups * d, n_rows), BF16), jax.ShapeDtypeStruct((groups, n_rows), F32),
                   jax.ShapeDtypeStruct((d, kv_all.shape[0]), BF16)),
        in_specs=[SMEM, VMEM, VMEM],
        out_specs=(VMEM, VMEM, VMEM),
        scratch_shapes=[pltpu.VMEM((groups, kw, n_rows), BF16), pltpu.VMEM((d, kv_all.shape[0]), BF16),
                        pltpu.VMEM((groups, half), F32), pltpu.VMEM((groups, half), F32), pltpu.VMEM((groups * d, half), F32)],
        cost_estimate=pl.CostEstimate(flops=32 * d * pairs, bytes_accessed=6 << 20, transcendentals=pairs),
        compiler_params=pltpu.CompilerParams(vmem_limit_bytes=40 << 20),
        interpret=interpret,
    )(rank_arr, qt, kv_all)


def attention_backward(rank_arr, qt, dot, ot, lse, kv_all, kt, h, kv_heads, n_shards, groups, d, interpret=False):
    n_rows = qt.shape[1]
    half = n_rows // 2
    kw = kv_all.shape[1] // 2
    pairs = groups * n_rows * n_rows * n_shards // 2
    return pl.pallas_call(
        functools.partial(backward_kernel, n_shards, groups, d, half, h, kv_heads),
        out_shape=(jax.ShapeDtypeStruct((groups * d, n_rows), BF16), jax.ShapeDtypeStruct((2 * d, kv_all.shape[0]), F32)),
        in_specs=[SMEM] + [VMEM] * 6,
        out_specs=(VMEM, VMEM),
        scratch_shapes=[pltpu.VMEM((groups, kw, n_rows), BF16), pltpu.VMEM((groups, kw, n_rows), BF16),
                        pltpu.VMEM((groups, n_rows), F32), pltpu.VMEM((groups * d, half), F32)],
        cost_estimate=pl.CostEstimate(flops=40 * d * pairs, bytes_accessed=8 << 20, transcendentals=pairs),
        compiler_params=pltpu.CompilerParams(vmem_limit_bytes=40 << 20),
        interpret=interpret,
    )(rank_arr, qt, dot, ot, lse, kv_all, kt)


def assemble_kernel(n_rows, source_ref, *refs):
    out_ref = refs[-1]
    n_slots = (len(refs) - 1) // 2
    for slot in range(n_slots):
        arrived = 0
        for ref in (refs[2 * slot], refs[2 * slot + 1]):
            for i in range(ref.shape[0]):
                blk = ref.shape[1]
                start = pl.multiple_of(slot * n_rows + source_ref[arrived] * blk, blk)
                out_ref[pl.ds(start, blk), :] = ref[i]
                arrived += 1


def assemble_kv(source_arr, pieces, n_rows, interpret=False):
    n_slots = len(pieces) // 2
    width = pieces[0].shape[2]
    return pl.pallas_call(
        functools.partial(assemble_kernel, n_rows),
        out_shape=jax.ShapeDtypeStruct((n_slots * n_rows, width), BF16),
        in_specs=[SMEM] + [VMEM] * len(pieces),
        out_specs=VMEM,
        cost_estimate=pl.CostEstimate(flops=1 << 20, bytes_accessed=4 * n_slots * n_rows * width, transcendentals=0),
        compiler_params=pltpu.CompilerParams(vmem_limit_bytes=16 << 20),
        name="assemble_kv",
        interpret=interpret,
    )(source_arr, *pieces)


def solution(mesh, interpret=False):
    n_cp, n_tp, n_dp = mesh.shape["cp"], mesh.shape["tp"], mesh.shape["dp"]
    ring = [*range(0, n_tp, 2), *reversed(range(1, n_tp, 2))]
    hop = [(ring[i], ring[(i + 1) % n_tp]) for i in range(n_tp)]
    source = [[ring[(ring.index(z) - s) % n_tp] for z in range(n_tp)] for s in range(n_tp)]

    def swap(arr, axis, bit):
        return lax.ppermute(arr, axis, [(i, i ^ bit) for i in range(mesh.shape[axis])])

    def pick(table, idx):
        out = jnp.int32(table[0])
        for i, value in enumerate(table[1:], 1):
            out = jnp.where(idx == i, value, out)
        return out

    def device_fn(x_blk, w_query, w_key, w_value, w_out, dy_blk):
        rank = lax.axis_index("cp")
        z = lax.axis_index("tp")
        model, q_heads, d = w_query.shape
        kv_heads = w_key.shape[1]
        groups = q_heads // kv_heads
        gd = groups * d
        blk = x_blk.shape[0]
        n_rows = blk * n_tp
        rank_arr = rank.astype(jnp.int32).reshape(1)
        wqt = w_query.transpose(1, 2, 0).reshape(q_heads * d, model)
        wkt = w_key.transpose(1, 2, 0).reshape(kv_heads * d, model)
        wvt = w_value.transpose(1, 2, 0).reshape(kv_heads * d, model)
        wkvt = jnp.concatenate([wkt, wvt], axis=0)
        wo = w_out.reshape(q_heads * d, model)

        n_plane = n_dp * n_cp
        plane = lax.axis_index("dp") * n_cp + rank
        w_heads = jnp.concatenate([part for h in range(kv_heads) for part in
                                   (wqt[h * gd:(h + 1) * gd], wkt[h * d:(h + 1) * d], wvt[h * d:(h + 1) * d])], axis=0)
        n_in = w_heads.shape[0] // n_plane
        n_out = wo.shape[0] // n_plane
        w_in_piece = lax.dynamic_slice(w_heads, (plane * n_in, 0), (n_in, model))
        wo_piece = lax.dynamic_slice(wo, (plane * n_out, 0), (n_out, model))

        wo_line, w_in_line = [wo_piece], [w_in_piece]

        def offset(step):
            return pick(source[step], z) * blk

        x_rows = jnp.zeros((n_rows, model), BF16)
        qt = jnp.zeros((q_heads * d, n_rows), BF16)
        kv_blocks, kv_moved = [], []
        held = x_blk

        def cp_exchange(arr):
            near = swap(arr, "cp", 1)
            far = swap(arr, "cp", 2)
            return [arr, near, far, swap(far, "cp", 1)]

        for step in range(n_tp):
            following = lax.ppermute(held, "tp", hop) if step < n_tp - 1 else None
            if step < n_tp - 1:
                w_in_line.append(lax.ppermute(w_in_line[-1], "tp", hop))
                wo_line.append(lax.ppermute(wo_line[-1], "tp", hop))
            kv_blocks.append(mm(held, wkvt, NT).astype(BF16))
            qt = lax.dynamic_update_slice(qt, mm(wqt, held, NT).astype(BF16) * BF16(d ** -0.5), (0, offset(step)))
            x_rows = lax.dynamic_update_slice(x_rows, held, (offset(step), 0))
            if step == n_tp - 2:
                kv_moved.append(cp_exchange(jnp.stack(kv_blocks)))
            if step == n_tp - 1:
                kv_moved.append(cp_exchange(kv_blocks[-1][None]))
            if following is not None:
                following, qt, x_rows, kv_blocks[-1], kv_moved = lax.optimization_barrier(
                    (following, qt, x_rows, kv_blocks[-1], kv_moved))
                held = following
        dy_first, w_in_line, wo_line, _ = lax.optimization_barrier((dy_blk, w_in_line, wo_line, held))
        w_in_full = lax.all_gather(jnp.concatenate(w_in_line, axis=0), ("dp", "cp"), axis=0, tiled=True)
        wo_full = lax.all_gather(jnp.concatenate(wo_line, axis=0), ("dp", "cp"), axis=0, tiled=True)
        source_arr = jnp.stack([pick(source[step], z) for step in range(n_tp)])
        pieces = [kv_moved[i][slot] for slot in range(n_cp) for i in range(2)]
        kv_all = assemble_kv(source_arr, pieces, n_rows, interpret)

        dy_rows = jnp.zeros((n_rows, model), BF16)
        dot = jnp.zeros((q_heads * d, n_rows), BF16)
        dy_held = dy_first
        fwd = []
        for step in range(n_tp):
            following = lax.ppermute(dy_held, "tp", hop) if step < n_tp - 1 else None
            dy_rows = lax.dynamic_update_slice(dy_rows, dy_held, (offset(step), 0))
            dot = lax.dynamic_update_slice(dot, mm(wo, dy_held, NT).astype(BF16), (0, offset(step)))
            if 1 <= step <= kv_heads:
                h = step - 1
                qt, kv_all, x_rows, dy_rows, dot = lax.optimization_barrier((qt, kv_all, x_rows, dy_rows, dot))
                fwd.append(attention_forward(rank_arr, qt, kv_all, h, kv_heads, n_cp, groups, d, interpret))
                if following is not None:
                    following, ot_h = lax.optimization_barrier((following, fwd[h][0]))
                    fwd[h] = (ot_h,) + tuple(fwd[h][1:])
            dy_held = following
        ot = jnp.concatenate([f[0] for f in fwd], axis=0)

        def exchange(arr_t):
            sent = [lax.dynamic_slice(arr_t, (0, lax.bitwise_xor(z, k) * blk), (arr_t.shape[0], blk)) for k in range(n_tp)]
            return [sent[0]] + [swap(sent[k], "tp", k) for k in range(1, n_tp)]

        def gathered_order(parts, n_pieces):
            stacked = jnp.stack(parts)
            feats, rows = stacked.shape[1:]
            by_arrival = jnp.stack([lax.dynamic_index_in_dim(stacked, lax.bitwise_xor(z, pick(source[t], z)), 0, keepdims=False)
                              for t in range(n_tp)])
            return by_arrival.reshape(n_tp, n_pieces, feats // n_pieces, rows).transpose(1, 0, 2, 3).reshape(n_tp * feats, rows)

        o_parts = exchange(ot)
        o_own = gathered_order(o_parts, n_plane)
        y_blk = mm(o_own, wo_full, TN).astype(BF16)

        dq_parts, dkv_parts, moved, waiting = [], [], [], None
        for h in range(kv_heads):
            dqt, dkv = attention_backward(rank_arr, qt, dot, fwd[h][0], fwd[h][1], kv_all, fwd[h][2],
                                          h, kv_heads, n_cp, groups, d, interpret)
            dq_parts.append(dqt)
            part = [dkv[:, j * n_rows:(j + 1) * n_rows] for j in range(n_cp)]
            if h < kv_heads - 1:
                moved.append(exchange(dqt))
                far_parts = [swap(part[j], "cp", j) for j in range(1, n_cp)]
                waiting = (part[0], far_parts)
            else:
                near = swap(jnp.concatenate([part[1], part[3]], axis=1), "cp", 1)
                if waiting is not None:
                    own, far_parts = waiting
                    dkv_own = functools.reduce(jnp.add, far_parts, own).astype(BF16)
                    dkv_parts.append(dkv_own)
                    moved.append(exchange(jnp.concatenate([dkv_own, dqt], axis=0)))
                else:
                    moved.append(exchange(dqt))
                far = swap(part[2] + near[:, n_rows:], "cp", 2)
                far, y_blk, moved[-1] = lax.optimization_barrier((far, y_blk, moved[-1]))
                dkv_own = (part[0] + near[:, :n_rows] + far).astype(BF16)
                dkv_parts.append(dkv_own)
                moved.append(exchange(dkv_own))
        n_early = (n_in * n_plane - dkv_parts[-1].shape[0]) // n_in
        early = [jnp.concatenate([m[k] for m in moved[:-1]], axis=0) for k in range(n_tp)]
        split = n_early * n_in * n_tp
        dx_early = mm(gathered_order([part[:n_early * n_in] for part in early], n_early), w_in_full[:split], TN)
        dx_early, last = lax.optimization_barrier((dx_early, moved[-1]))
        late = [jnp.concatenate([early[k][n_early * n_in:], last[k]], axis=0) for k in range(n_tp)]
        dx_blk = (dx_early + mm(gathered_order(late, n_plane - n_early), w_in_full[split:], TN)).astype(BF16)

        def weight_layout(grad_t):
            return grad_t.reshape(-1, d, model).transpose(2, 0, 1)[None]

        dk_dv = jnp.concatenate([part[:d] for part in dkv_parts] + [part[d:] for part in dkv_parts], axis=0)
        grad_wq = mm(jnp.concatenate(dq_parts, axis=0), x_rows).astype(BF16)
        grad_wkv = mm(dk_dv, x_rows).astype(BF16)
        grad_wo = mm(ot, dy_rows).astype(BF16).reshape(q_heads, d, model)
        return (y_blk, dx_blk, weight_layout(grad_wq), weight_layout(grad_wkv[:kv_heads * d]), weight_layout(grad_wkv[kv_heads * d:]),
                grad_wo[None])

    return jax.shard_map(device_fn, mesh=mesh,
                         in_specs=(ROW_SPEC, HEAD_SPEC, HEAD_SPEC, HEAD_SPEC, OUT_W_SPEC, ROW_SPEC),
                         out_specs=(ROW_SPEC, ROW_SPEC, GRAD_SPEC, GRAD_SPEC, GRAD_SPEC, GRAD_OUT_SPEC),
                         check_vma=False)
```

```python
import functools

import jax
import jax.numpy as jnp
from jax import lax
from jax.experimental import pallas as pl
from jax.experimental.pallas import tpu as pltpu
from jax.sharding import PartitionSpec as P


ROW_SPEC = P(("dp", "cp", "tp"), None)
HEAD_SPEC = P(None, "tp", None)
OUT_W_SPEC = P("tp", None, None)
GRAD_SPEC = P(("dp", "cp"), None, "tp", None)
GRAD_OUT_SPEC = P(("dp", "cp"), "tp", None, None)
TN = (((0,), (0,)), ((), ()))
NT = (((1,), (1,)), ((), ()))
F32 = jnp.float32
BF16 = jnp.bfloat16


def mm(lhs, rhs, dims=(((1,), (0,)), ((), ()))):
    return lax.dot_general(lhs, rhs, dims, preferred_element_type=F32)


def chunk_offset(chunk, rank, n_shards, half):
    shard = jnp.where(chunk < n_shards, chunk, 2 * n_shards - 1 - chunk)
    upper = jnp.where(chunk < n_shards, 0, half)
    return pl.multiple_of(lax.bitwise_xor(shard, rank) * (2 * half) + upper, half)


def forward_kernel(n_shards, groups, d, half, h, kv_heads, rank_ref, qt_ref, kv_ref, ot_ref, lse_ref, kt_ref, q_pad, vt_s, m_s, l_s, acc_s):
    rank = rank_ref[0]
    kw = kv_heads * d
    sub = half // 2
    q_pad[...] = jnp.zeros_like(q_pad)
    for g in range(groups):
        q_pad[g, h * d:(h + 1) * d, :] = qt_ref[(h * groups + g) * d:(h * groups + g + 1) * d, :]

    def transpose_chunk(i, carry):
        rows = pl.ds(pl.multiple_of(i * half, half), half)
        kt_ref[:, rows] = kv_ref[rows, :kw].T[h * d:(h + 1) * d, :]
        vt_s[:, rows] = kv_ref[rows, kw:].T[h * d:(h + 1) * d, :]
        return carry

    lax.fori_loop(0, kv_ref.shape[0] // half, transpose_chunk, 0)

    def update(g, q_start, q_lo, q_len, k_off, k_len, masked):
        cols = slice(q_lo, q_lo + q_len)
        scores = mm(kv_ref[pl.ds(k_off, k_len), :kw], q_pad[g, :, q_start + q_lo:q_start + q_lo + q_len])
        if masked:
            k_id = lax.broadcasted_iota(jnp.int32, scores.shape, 0)
            q_id = lax.broadcasted_iota(jnp.int32, scores.shape, 1)
            scores = jnp.where(q_id >= k_id, scores, -jnp.inf)
        m_old = m_s[g:g + 1, cols]
        m_new = jnp.maximum(m_old, jnp.max(scores, axis=0, keepdims=True))
        prob = jnp.exp(scores - m_new)
        factor = jnp.exp(m_old - m_new)
        m_s[g:g + 1, cols] = m_new
        l_s[g:g + 1, cols] = l_s[g:g + 1, cols] * factor + jnp.sum(prob, axis=0, keepdims=True)
        pv = mm(vt_s[:, pl.ds(k_off, k_len)], prob.astype(BF16))
        acc_s[g * d:(g + 1) * d, cols] = acc_s[g * d:(g + 1) * d, cols] * factor + pv

    for q_half in range(2):
        q_start = q_half * half
        n_full = rank if q_half == 0 else 2 * n_shards - 1 - rank
        m_s[...] = jnp.full_like(m_s, -jnp.inf)
        l_s[...] = jnp.zeros_like(l_s)
        acc_s[...] = jnp.zeros_like(acc_s)
        off = chunk_offset(n_full, rank, n_shards, half)
        for g in range(groups):
            update(g, q_start, 0, half, off, sub, True)
        for g in range(groups):
            update(g, q_start, sub, sub, pl.multiple_of(off + sub, sub), sub, True)

        def full_block(chunk, carry):
            k_off = chunk_offset(chunk, rank, n_shards, half)
            for g in range(groups):
                update(g, q_start, 0, half, k_off, half, False)
            return carry

        lax.fori_loop(0, n_full, full_block, 0)
        for g in range(groups):
            l_row = l_s[g:g + 1, :]
            ot_ref[g * d:(g + 1) * d, q_start:q_start + half] = (acc_s[g * d:(g + 1) * d, :] / l_row).astype(BF16)
            lse_ref[g:g + 1, q_start:q_start + half] = m_s[g:g + 1, :] + jnp.log(l_row)


def backward_kernel(n_shards, groups, d, half, h, kv_heads, rank_ref, qt_ref, dot_ref, ot_ref, lse_ref, kv_ref, kt_ref,
                    dqt_ref, dkv_ref, q_pad, do_pad, delta_s, dq_s):
    rank = rank_ref[0]
    kw = kv_heads * d
    sub = half // 2
    q_pad[...] = jnp.zeros_like(q_pad)
    do_pad[...] = jnp.zeros_like(do_pad)
    for g in range(groups):
        rows = slice(g * d, (g + 1) * d)
        full = slice((h * groups + g) * d, (h * groups + g + 1) * d)
        q_pad[g, h * d:(h + 1) * d, :] = qt_ref[full, :]
        do_pad[g, h * d:(h + 1) * d, :] = dot_ref[full, :]
        delta_s[g:g + 1, :] = jnp.sum(dot_ref[full, :].astype(F32) * ot_ref[rows, :].astype(F32), axis=0, keepdims=True)
    dkv_ref[...] = jnp.zeros_like(dkv_ref)

    def update(q_start, q_lo, q_len, k_off, k_len, masked):
        lo = q_start + q_lo
        cols = slice(lo, lo + q_len)
        k_blk = kv_ref[pl.ds(k_off, k_len), :kw]
        v_blk = kv_ref[pl.ds(k_off, k_len), kw:]
        dk_sum, dv_sum = None, None
        for g in range(groups):
            rows = slice(g * d, (g + 1) * d)
            full = slice((h * groups + g) * d, (h * groups + g + 1) * d)
            scores = mm(k_blk, q_pad[g, :, cols])
            prob = jnp.exp(scores - lse_ref[g:g + 1, cols])
            if masked:
                k_id = lax.broadcasted_iota(jnp.int32, scores.shape, 0)
                q_id = lax.broadcasted_iota(jnp.int32, scores.shape, 1)
                prob = jnp.where(q_id >= k_id, prob, 0.0)
            d_prob = mm(v_blk, do_pad[g, :, cols])
            d_score = (prob * (d_prob - delta_s[g:g + 1, cols])).astype(BF16)
            dv = mm(dot_ref[full, cols], prob.astype(BF16), NT)
            dk = mm(qt_ref[full, cols], d_score, NT)
            dk_sum = dk if dk_sum is None else dk_sum + dk
            dv_sum = dv if dv_sum is None else dv_sum + dv
            dq_s[rows, q_lo:q_lo + q_len] += mm(kt_ref[:, pl.ds(k_off, k_len)], d_score)
        dkv_ref[:d, pl.ds(k_off, k_len)] += dk_sum
        dkv_ref[d:, pl.ds(k_off, k_len)] += dv_sum

    for q_half in range(2):
        q_start = q_half * half
        n_full = rank if q_half == 0 else 2 * n_shards - 1 - rank
        dq_s[...] = jnp.zeros_like(dq_s)
        off = chunk_offset(n_full, rank, n_shards, half)
        update(q_start, 0, half, off, sub, True)
        update(q_start, sub, sub, pl.multiple_of(off + sub, sub), sub, True)

        def full_block(chunk, carry):
            update(q_start, 0, half, chunk_offset(chunk, rank, n_shards, half), half, False)
            return carry

        lax.fori_loop(0, n_full, full_block, 0)
        dqt_ref[:, q_start:q_start + half] = (dq_s[...] * (d ** -0.5)).astype(BF16)


VMEM = pl.BlockSpec(memory_space=pltpu.VMEM)
SMEM = pl.BlockSpec(memory_space=pltpu.SMEM)


def attention_forward(rank_arr, qt, kv_all, h, kv_heads, n_shards, groups, d, interpret=False):
    n_rows = qt.shape[1]
    half = n_rows // 2
    kw = kv_all.shape[1] // 2
    pairs = groups * n_rows * n_rows * n_shards // 2
    return pl.pallas_call(
        functools.partial(forward_kernel, n_shards, groups, d, half, h, kv_heads),
        out_shape=(jax.ShapeDtypeStruct((groups * d, n_rows), BF16), jax.ShapeDtypeStruct((groups, n_rows), F32),
                   jax.ShapeDtypeStruct((d, kv_all.shape[0]), BF16)),
        in_specs=[SMEM, VMEM, VMEM],
        out_specs=(VMEM, VMEM, VMEM),
        scratch_shapes=[pltpu.VMEM((groups, kw, n_rows), BF16), pltpu.VMEM((d, kv_all.shape[0]), BF16),
                        pltpu.VMEM((groups, half), F32), pltpu.VMEM((groups, half), F32), pltpu.VMEM((groups * d, half), F32)],
        cost_estimate=pl.CostEstimate(flops=32 * d * pairs, bytes_accessed=6 << 20, transcendentals=pairs),
        compiler_params=pltpu.CompilerParams(vmem_limit_bytes=40 << 20),
        interpret=interpret,
    )(rank_arr, qt, kv_all)


def attention_backward(rank_arr, qt, dot, ot, lse, kv_all, kt, h, kv_heads, n_shards, groups, d, interpret=False):
    n_rows = qt.shape[1]
    half = n_rows // 2
    kw = kv_all.shape[1] // 2
    pairs = groups * n_rows * n_rows * n_shards // 2
    return pl.pallas_call(
        functools.partial(backward_kernel, n_shards, groups, d, half, h, kv_heads),
        out_shape=(jax.ShapeDtypeStruct((groups * d, n_rows), BF16), jax.ShapeDtypeStruct((2 * d, kv_all.shape[0]), F32)),
        in_specs=[SMEM] + [VMEM] * 6,
        out_specs=(VMEM, VMEM),
        scratch_shapes=[pltpu.VMEM((groups, kw, n_rows), BF16), pltpu.VMEM((groups, kw, n_rows), BF16),
                        pltpu.VMEM((groups, n_rows), F32), pltpu.VMEM((groups * d, half), F32)],
        cost_estimate=pl.CostEstimate(flops=40 * d * pairs, bytes_accessed=8 << 20, transcendentals=pairs),
        compiler_params=pltpu.CompilerParams(vmem_limit_bytes=40 << 20),
        interpret=interpret,
    )(rank_arr, qt, dot, ot, lse, kv_all, kt)


def assemble_kernel(n_rows, source_ref, *refs):
    out_ref = refs[-1]
    n_slots = (len(refs) - 1) // 2
    for slot in range(n_slots):
        arrived = 0
        for ref in (refs[2 * slot], refs[2 * slot + 1]):
            for i in range(ref.shape[0]):
                blk = ref.shape[1]
                start = pl.multiple_of(slot * n_rows + source_ref[arrived] * blk, blk)
                out_ref[pl.ds(start, blk), :] = ref[i]
                arrived += 1


def assemble_kv(source_arr, pieces, n_rows, interpret=False):
    n_slots = len(pieces) // 2
    width = pieces[0].shape[2]
    return pl.pallas_call(
        functools.partial(assemble_kernel, n_rows),
        out_shape=jax.ShapeDtypeStruct((n_slots * n_rows, width), BF16),
        in_specs=[SMEM] + [VMEM] * len(pieces),
        out_specs=VMEM,
        cost_estimate=pl.CostEstimate(flops=1 << 20, bytes_accessed=4 * n_slots * n_rows * width, transcendentals=0),
        compiler_params=pltpu.CompilerParams(vmem_limit_bytes=16 << 20),
        name="assemble_kv",
        interpret=interpret,
    )(source_arr, *pieces)


def weight_grads_kernel(dq0_ref, dq1_ref, dkv0_ref, dkv1_ref, x_ref, gq_ref, gk_ref, gv_ref):
    x_cols = x_ref[...]
    half_q = dq0_ref.shape[0]
    d = dkv0_ref.shape[0] // 2
    gq_ref[:half_q, :] = mm(dq0_ref[...], x_cols).astype(BF16)
    gq_ref[half_q:, :] = mm(dq1_ref[...], x_cols).astype(BF16)
    for i, ref in enumerate((dkv0_ref, dkv1_ref)):
        both = mm(ref[...], x_cols).astype(BF16)
        gk_ref[i * d:(i + 1) * d, :] = both[:d]
        gv_ref[i * d:(i + 1) * d, :] = both[d:]


def weight_grads(dq_parts, dkv_parts, x_rows, interpret=False):
    n_rows, model = x_rows.shape
    cols = min(512, model)
    q_feats = 2 * dq_parts[0].shape[0]
    kv_feats = dkv_parts[0].shape[0]
    whole = lambda arr: pl.BlockSpec(arr.shape, lambda i: (0, 0))
    block = lambda feats: pl.BlockSpec((feats, cols), lambda i: (0, i))
    return pl.pallas_call(
        weight_grads_kernel,
        grid=(model // cols,),
        out_shape=tuple(jax.ShapeDtypeStruct((feats, model), BF16) for feats in (q_feats, kv_feats, kv_feats)),
        in_specs=[whole(dq_parts[0])] * 2 + [whole(dkv_parts[0])] * 2 + [block(n_rows)],
        out_specs=(block(q_feats), block(kv_feats), block(kv_feats)),
        cost_estimate=pl.CostEstimate(flops=2 * (q_feats + 2 * kv_feats) * n_rows * model, bytes_accessed=10 << 20, transcendentals=0),
        compiler_params=pltpu.CompilerParams(vmem_limit_bytes=32 << 20),
        name="weight_grads",
        interpret=interpret,
    )(*dq_parts, *dkv_parts, x_rows)


def solution(mesh, interpret=False):
    n_cp, n_tp, n_dp = mesh.shape["cp"], mesh.shape["tp"], mesh.shape["dp"]
    ring = [*range(0, n_tp, 2), *reversed(range(1, n_tp, 2))]
    hop = [(ring[i], ring[(i + 1) % n_tp]) for i in range(n_tp)]
    source = [[ring[(ring.index(z) - s) % n_tp] for z in range(n_tp)] for s in range(n_tp)]

    def swap(arr, axis, bit):
        return lax.ppermute(arr, axis, [(i, i ^ bit) for i in range(mesh.shape[axis])])

    def pick(table, idx):
        out = jnp.int32(table[0])
        for i, value in enumerate(table[1:], 1):
            out = jnp.where(idx == i, value, out)
        return out

    def device_fn(x_blk, w_query, w_key, w_value, w_out, dy_blk):
        rank = lax.axis_index("cp")
        z = lax.axis_index("tp")
        model, q_heads, d = w_query.shape
        kv_heads = w_key.shape[1]
        groups = q_heads // kv_heads
        gd = groups * d
        blk = x_blk.shape[0]
        n_rows = blk * n_tp
        rank_arr = rank.astype(jnp.int32).reshape(1)
        wqt = w_query.transpose(1, 2, 0).reshape(q_heads * d, model)
        wkt = w_key.transpose(1, 2, 0).reshape(kv_heads * d, model)
        wvt = w_value.transpose(1, 2, 0).reshape(kv_heads * d, model)
        wkvt = jnp.concatenate([wkt, wvt], axis=0)
        wo = w_out.reshape(q_heads * d, model)

        n_plane = n_dp * n_cp
        plane = lax.axis_index("dp") * n_cp + rank
        w_heads = jnp.concatenate([part for h in range(kv_heads) for part in
                                   (wqt[h * gd:(h + 1) * gd], wkt[h * d:(h + 1) * d], wvt[h * d:(h + 1) * d])], axis=0)
        n_in = w_heads.shape[0] // n_plane
        n_out = wo.shape[0] // n_plane
        w_in_piece = lax.dynamic_slice(w_heads, (plane * n_in, 0), (n_in, model))
        wo_piece = lax.dynamic_slice(wo, (plane * n_out, 0), (n_out, model))

        w_in_line = [w_in_piece]

        def offset(step):
            return pick(source[step], z) * blk

        x_rows = jnp.zeros((n_rows, model), BF16)
        qt = jnp.zeros((q_heads * d, n_rows), BF16)
        kv_blocks, kv_moved = [], []
        held = x_blk

        def cp_exchange(arr):
            near = swap(arr, "cp", 1)
            far = swap(arr, "cp", 2)
            return [arr, near, far, swap(far, "cp", 1)]

        for step in range(n_tp):
            following = lax.ppermute(held, "tp", hop) if step < n_tp - 1 else None
            if step < n_tp - 1:
                w_in_line.append(lax.ppermute(w_in_line[-1], "tp", hop))
            kv_blocks.append(mm(held, wkvt, NT).astype(BF16))
            qt = lax.dynamic_update_slice(qt, mm(wqt, held, NT).astype(BF16) * BF16(d ** -0.5), (0, offset(step)))
            x_rows = lax.dynamic_update_slice(x_rows, held, (offset(step), 0))
            if step == n_tp - 2:
                kv_moved.append(cp_exchange(jnp.stack(kv_blocks)))
            if step == n_tp - 1:
                kv_moved.append(cp_exchange(kv_blocks[-1][None]))
            if following is not None:
                following, qt, x_rows, kv_blocks[-1], kv_moved, w_in_line[:-1] = lax.optimization_barrier(
                    (following, qt, x_rows, kv_blocks[-1], kv_moved, w_in_line[:-1]))
                held = following
        dy_first, _ = lax.optimization_barrier((dy_blk, held))
        w_in_line, _ = lax.optimization_barrier((w_in_line, kv_blocks[-1]))
        w_in_line = jnp.concatenate(w_in_line, axis=0)
        w_in_full = lax.all_gather(w_in_line, ("dp", "cp"), axis=0, tiled=True)
        qt, w_in_line = lax.optimization_barrier((qt, w_in_line))
        source_arr = jnp.stack([pick(source[step], z) for step in range(n_tp)])
        pieces = [kv_moved[i][slot] for slot in range(n_cp) for i in range(2)]
        kv_all = assemble_kv(source_arr, pieces, n_rows, interpret)

        dy_rows = jnp.zeros((n_rows, model), BF16)
        dot = jnp.zeros((q_heads * d, n_rows), BF16)
        dy_held = dy_first
        fwd = []
        for step in range(n_tp):
            following = lax.ppermute(dy_held, "tp", hop) if step < n_tp - 1 else None
            dy_rows = lax.dynamic_update_slice(dy_rows, dy_held, (offset(step), 0))
            dot = lax.dynamic_update_slice(dot, mm(wo, dy_held, NT).astype(BF16), (0, offset(step)))
            if 1 <= step <= kv_heads:
                h = step - 1
                qt, kv_all, x_rows, dy_rows, dot = lax.optimization_barrier((qt, kv_all, x_rows, dy_rows, dot))
                fwd.append(attention_forward(rank_arr, qt, kv_all, h, kv_heads, n_cp, groups, d, interpret))
                if following is not None:
                    following, ot_h = lax.optimization_barrier((following, fwd[h][0]))
                    fwd[h] = (ot_h,) + tuple(fwd[h][1:])
            dy_last, dy_held = dy_held, following
        ot = jnp.concatenate([f[0] for f in fwd], axis=0)

        def exchange(arr_t):
            sent = [lax.dynamic_slice(arr_t, (0, lax.bitwise_xor(z, k) * blk), (arr_t.shape[0], blk)) for k in range(n_tp)]
            return [sent[0]] + [swap(sent[k], "tp", k) for k in range(1, n_tp)]

        def plane_order(parts, n_pieces):
            feats, rows = parts.shape[1:]
            return parts.reshape(n_tp, n_pieces, feats // n_pieces, rows).transpose(1, 0, 2, 3).reshape(n_tp * feats, rows)

        def by_arrival(parts):
            stacked = jnp.stack(parts)
            return jnp.stack([lax.dynamic_index_in_dim(stacked, lax.bitwise_xor(z, pick(source[t], z)), 0, keepdims=False)
                              for t in range(n_tp)])

        wo_piece, _ = lax.optimization_barrier((wo_piece, dy_last))
        wo_line = jnp.concatenate([wo_piece] + [swap(wo_piece, "tp", k) for k in range(1, n_tp)], axis=0)
        o_parts = exchange(ot)

        dq_parts, dkv_parts, moved, waiting = [], [], [], None
        for h in range(kv_heads):
            dqt, dkv = attention_backward(rank_arr, qt, dot, fwd[h][0], fwd[h][1], kv_all, fwd[h][2],
                                          h, kv_heads, n_cp, groups, d, interpret)
            dq_parts.append(dqt)
            part = [dkv[:, j * n_rows:(j + 1) * n_rows] for j in range(n_cp)]
            if h < kv_heads - 1:
                moved.append(exchange(dqt))
                far_parts = [swap(part[j], "cp", j) for j in range(1, n_cp)]
                waiting = (part[0], far_parts)
                if h == 0:
                    wo_line, dqt, w_in_full = lax.optimization_barrier((wo_line, dqt, w_in_full))
                    wo_full = lax.all_gather(wo_line, ("dp", "cp"), axis=0, tiled=True)
            else:
                near = swap(jnp.concatenate([part[1], part[3]], axis=1), "cp", 1)
                if waiting is not None:
                    own, far_parts = waiting
                    dkv_own = functools.reduce(jnp.add, far_parts, own).astype(BF16)
                    dkv_parts.append(dkv_own)
                    moved.append(exchange(jnp.concatenate([dkv_own, dqt], axis=0)))
                else:
                    moved.append(exchange(dqt))
                far = swap(part[2] + near[:, n_rows:], "cp", 2)
                dkv_own = (part[0] + near[:, :n_rows] + far).astype(BF16)
                dkv_parts.append(dkv_own)
                moved.append(exchange(dkv_own))
        n_early = (n_in * n_plane - dkv_parts[-1].shape[0]) // n_in
        early = [jnp.concatenate([m[k] for m in moved[:-1]], axis=0) for k in range(n_tp)]
        split = n_early * n_in * n_tp
        dx_early = mm(plane_order(by_arrival([part[:n_early * n_in] for part in early]), n_early), w_in_full[:split], TN)
        y_blk = mm(plane_order(jnp.stack(o_parts), n_plane), wo_full, TN).astype(BF16)
        last = moved[-1]
        late = [jnp.concatenate([early[k][n_early * n_in:], last[k]], axis=0) for k in range(n_tp)]
        dx_blk = (dx_early + mm(plane_order(by_arrival(late), n_plane - n_early), w_in_full[split:], TN)).astype(BF16)

        def weight_layout(grad_t):
            return grad_t.reshape(-1, d, model).transpose(2, 0, 1)[None]

        grad_wq, grad_wk, grad_wv = weight_grads(dq_parts, dkv_parts, x_rows, interpret)
        grad_wo = mm(ot, dy_rows).astype(BF16).reshape(q_heads, d, model)
        return (y_blk, dx_blk, weight_layout(grad_wq), weight_layout(grad_wk), weight_layout(grad_wv),
                grad_wo[None])

    return jax.shard_map(device_fn, mesh=mesh,
                         in_specs=(ROW_SPEC, HEAD_SPEC, HEAD_SPEC, HEAD_SPEC, OUT_W_SPEC, ROW_SPEC),
                         out_specs=(ROW_SPEC, ROW_SPEC, GRAD_SPEC, GRAD_SPEC, GRAD_SPEC, GRAD_OUT_SPEC),
                         check_vma=False)
```

```python
import functools

import jax
import jax.numpy as jnp
from jax import lax
from jax.experimental import pallas as pl
from jax.experimental.pallas import tpu as pltpu
from jax.sharding import PartitionSpec as P


ROW_SPEC = P(("dp", "cp", "tp"), None)
HEAD_SPEC = P(None, "tp", None)
OUT_W_SPEC = P("tp", None, None)
GRAD_SPEC = P(("dp", "cp"), None, "tp", None)
GRAD_OUT_SPEC = P(("dp", "cp"), "tp", None, None)
TN = (((0,), (0,)), ((), ()))
NT = (((1,), (1,)), ((), ()))
F32 = jnp.float32
BF16 = jnp.bfloat16


def mm(lhs, rhs, dims=(((1,), (0,)), ((), ()))):
    return lax.dot_general(lhs, rhs, dims, preferred_element_type=F32)


def chunk_offset(chunk, rank, n_shards, half):
    shard = jnp.where(chunk < n_shards, chunk, 2 * n_shards - 1 - chunk)
    upper = jnp.where(chunk < n_shards, 0, half)
    return pl.multiple_of(lax.bitwise_xor(shard, rank) * (2 * half) + upper, half)


def forward_kernel(n_shards, groups, d, half, h, kv_heads, rank_ref, qt_ref, kv_ref, ot_ref, lse_ref, kt_ref, q_pad, vt_s, m_s, l_s, acc_s):
    rank = rank_ref[0]
    kw = kv_heads * d
    sub = half // 2
    q_pad[...] = jnp.zeros_like(q_pad)
    for g in range(groups):
        q_pad[g, h * d:(h + 1) * d, :] = qt_ref[(h * groups + g) * d:(h * groups + g + 1) * d, :]

    def transpose_chunk(i, carry):
        rows = pl.ds(pl.multiple_of(i * half, half), half)
        kt_ref[:, rows] = kv_ref[rows, :kw].T[h * d:(h + 1) * d, :]
        vt_s[:, rows] = kv_ref[rows, kw:].T[h * d:(h + 1) * d, :]
        return carry

    lax.fori_loop(0, kv_ref.shape[0] // half, transpose_chunk, 0)

    def update(g, q_start, q_lo, q_len, k_off, k_len, masked):
        cols = slice(q_lo, q_lo + q_len)
        scores = mm(kv_ref[pl.ds(k_off, k_len), :kw], q_pad[g, :, pl.ds(pl.multiple_of(q_start + q_lo, sub), q_len)])
        if masked:
            k_id = lax.broadcasted_iota(jnp.int32, scores.shape, 0)
            q_id = lax.broadcasted_iota(jnp.int32, scores.shape, 1)
            scores = jnp.where(q_id >= k_id, scores, -jnp.inf)
        m_old = m_s[g:g + 1, cols]
        m_new = jnp.maximum(m_old, jnp.max(scores, axis=0, keepdims=True))
        prob = jnp.exp(scores - m_new)
        factor = jnp.exp(m_old - m_new)
        m_s[g:g + 1, cols] = m_new
        l_s[g:g + 1, cols] = l_s[g:g + 1, cols] * factor + jnp.sum(prob, axis=0, keepdims=True)
        pv = mm(vt_s[:, pl.ds(k_off, k_len)], prob.astype(BF16))
        acc_s[g * d:(g + 1) * d, cols] = acc_s[g * d:(g + 1) * d, cols] * factor + pv

    def query_half(q_half, done):
        q_start = pl.multiple_of(q_half * half, half)
        n_full = jnp.where(q_half == 0, rank, 2 * n_shards - 1 - rank)
        m_s[...] = jnp.full_like(m_s, -jnp.inf)
        l_s[...] = jnp.zeros_like(l_s)
        acc_s[...] = jnp.zeros_like(acc_s)
        off = chunk_offset(n_full, rank, n_shards, half)
        for g in range(groups):
            update(g, q_start, 0, half, off, sub, True)
        for g in range(groups):
            update(g, q_start, sub, sub, pl.multiple_of(off + sub, sub), sub, True)

        def full_block(chunk, carry):
            k_off = chunk_offset(chunk, rank, n_shards, half)
            for g in range(groups):
                update(g, q_start, 0, half, k_off, half, False)
            return carry

        lax.fori_loop(0, n_full, full_block, 0)
        for g in range(groups):
            l_row = l_s[g:g + 1, :]
            ot_ref[g * d:(g + 1) * d, pl.ds(q_start, half)] = (acc_s[g * d:(g + 1) * d, :] / l_row).astype(BF16)
            lse_ref[g:g + 1, pl.ds(q_start, half)] = m_s[g:g + 1, :] + jnp.log(l_row)
        return done

    lax.fori_loop(0, 2, query_half, 0)


def backward_kernel(n_shards, groups, d, half, h, kv_heads, rank_ref, qt_ref, dot_ref, ot_ref, lse_ref, kv_ref, kt_ref,
                    dqt_ref, dkv_ref, q_pad, do_pad, delta_s, dq_s):
    rank = rank_ref[0]
    kw = kv_heads * d
    sub = half // 2
    q_pad[...] = jnp.zeros_like(q_pad)
    do_pad[...] = jnp.zeros_like(do_pad)
    for g in range(groups):
        rows = slice(g * d, (g + 1) * d)
        full = slice((h * groups + g) * d, (h * groups + g + 1) * d)
        q_pad[g, h * d:(h + 1) * d, :] = qt_ref[full, :]
        do_pad[g, h * d:(h + 1) * d, :] = dot_ref[full, :]
        delta_s[g:g + 1, :] = jnp.sum(dot_ref[full, :].astype(F32) * ot_ref[rows, :].astype(F32), axis=0, keepdims=True)
    dkv_ref[...] = jnp.zeros_like(dkv_ref)

    def update(q_start, q_lo, q_len, k_off, k_len, masked):
        cols = pl.ds(pl.multiple_of(q_start + q_lo, sub), q_len)
        k_blk = kv_ref[pl.ds(k_off, k_len), :kw]
        v_blk = kv_ref[pl.ds(k_off, k_len), kw:]
        dk_sum, dv_sum = None, None
        for g in range(groups):
            rows = slice(g * d, (g + 1) * d)
            full = slice((h * groups + g) * d, (h * groups + g + 1) * d)
            scores = mm(k_blk, q_pad[g, :, cols])
            prob = jnp.exp(scores - lse_ref[g:g + 1, cols])
            if masked:
                k_id = lax.broadcasted_iota(jnp.int32, scores.shape, 0)
                q_id = lax.broadcasted_iota(jnp.int32, scores.shape, 1)
                prob = jnp.where(q_id >= k_id, prob, 0.0)
            d_prob = mm(v_blk, do_pad[g, :, cols])
            d_score = (prob * (d_prob - delta_s[g:g + 1, cols])).astype(BF16)
            dv = mm(dot_ref[full, cols], prob.astype(BF16), NT)
            dk = mm(qt_ref[full, cols], d_score, NT)
            dk_sum = dk if dk_sum is None else dk_sum + dk
            dv_sum = dv if dv_sum is None else dv_sum + dv
            dq_s[rows, q_lo:q_lo + q_len] += mm(kt_ref[:, pl.ds(k_off, k_len)], d_score)
        dkv_ref[:d, pl.ds(k_off, k_len)] += dk_sum
        dkv_ref[d:, pl.ds(k_off, k_len)] += dv_sum

    def query_half(q_half, done):
        q_start = pl.multiple_of(q_half * half, half)
        n_full = jnp.where(q_half == 0, rank, 2 * n_shards - 1 - rank)
        dq_s[...] = jnp.zeros_like(dq_s)
        off = chunk_offset(n_full, rank, n_shards, half)
        update(q_start, 0, half, off, sub, True)
        update(q_start, sub, sub, pl.multiple_of(off + sub, sub), sub, True)

        def full_block(chunk, carry):
            update(q_start, 0, half, chunk_offset(chunk, rank, n_shards, half), half, False)
            return carry

        lax.fori_loop(0, n_full, full_block, 0)
        dqt_ref[:, pl.ds(q_start, half)] = (dq_s[...] * (d ** -0.5)).astype(BF16)
        return done

    lax.fori_loop(0, 2, query_half, 0)


VMEM = pl.BlockSpec(memory_space=pltpu.VMEM)
SMEM = pl.BlockSpec(memory_space=pltpu.SMEM)


def attention_forward(rank_arr, qt, kv_all, h, kv_heads, n_shards, groups, d, interpret=False):
    n_rows = qt.shape[1]
    half = n_rows // 2
    kw = kv_all.shape[1] // 2
    pairs = groups * n_rows * n_rows * n_shards // 2
    return pl.pallas_call(
        functools.partial(forward_kernel, n_shards, groups, d, half, h, kv_heads),
        out_shape=(jax.ShapeDtypeStruct((groups * d, n_rows), BF16), jax.ShapeDtypeStruct((groups, n_rows), F32),
                   jax.ShapeDtypeStruct((d, kv_all.shape[0]), BF16)),
        in_specs=[SMEM, VMEM, VMEM],
        out_specs=(VMEM, VMEM, VMEM),
        scratch_shapes=[pltpu.VMEM((groups, kw, n_rows), BF16), pltpu.VMEM((d, kv_all.shape[0]), BF16),
                        pltpu.VMEM((groups, half), F32), pltpu.VMEM((groups, half), F32), pltpu.VMEM((groups * d, half), F32)],
        cost_estimate=pl.CostEstimate(flops=32 * d * pairs, bytes_accessed=6 << 20, transcendentals=pairs),
        compiler_params=pltpu.CompilerParams(vmem_limit_bytes=40 << 20),
        interpret=interpret,
    )(rank_arr, qt, kv_all)


def attention_backward(rank_arr, qt, dot, ot, lse, kv_all, kt, h, kv_heads, n_shards, groups, d, interpret=False):
    n_rows = qt.shape[1]
    half = n_rows // 2
    kw = kv_all.shape[1] // 2
    pairs = groups * n_rows * n_rows * n_shards // 2
    return pl.pallas_call(
        functools.partial(backward_kernel, n_shards, groups, d, half, h, kv_heads),
        out_shape=(jax.ShapeDtypeStruct((groups * d, n_rows), BF16), jax.ShapeDtypeStruct((2 * d, kv_all.shape[0]), F32)),
        in_specs=[SMEM] + [VMEM] * 6,
        out_specs=(VMEM, VMEM),
        scratch_shapes=[pltpu.VMEM((groups, kw, n_rows), BF16), pltpu.VMEM((groups, kw, n_rows), BF16),
                        pltpu.VMEM((groups, n_rows), F32), pltpu.VMEM((groups * d, half), F32)],
        cost_estimate=pl.CostEstimate(flops=40 * d * pairs, bytes_accessed=8 << 20, transcendentals=pairs),
        compiler_params=pltpu.CompilerParams(vmem_limit_bytes=40 << 20),
        interpret=interpret,
    )(rank_arr, qt, dot, ot, lse, kv_all, kt)


def assemble_kernel(n_rows, source_ref, *refs):
    out_ref = refs[-1]
    n_slots = (len(refs) - 1) // 2
    for slot in range(n_slots):
        arrived = 0
        for ref in (refs[2 * slot], refs[2 * slot + 1]):
            for i in range(ref.shape[0]):
                blk = ref.shape[1]
                start = pl.multiple_of(slot * n_rows + source_ref[arrived] * blk, blk)
                out_ref[pl.ds(start, blk), :] = ref[i]
                arrived += 1


def assemble_kv(source_arr, pieces, n_rows, interpret=False):
    n_slots = len(pieces) // 2
    width = pieces[0].shape[2]
    return pl.pallas_call(
        functools.partial(assemble_kernel, n_rows),
        out_shape=jax.ShapeDtypeStruct((n_slots * n_rows, width), BF16),
        in_specs=[SMEM] + [VMEM] * len(pieces),
        out_specs=VMEM,
        cost_estimate=pl.CostEstimate(flops=1 << 20, bytes_accessed=4 * n_slots * n_rows * width, transcendentals=0),
        compiler_params=pltpu.CompilerParams(vmem_limit_bytes=16 << 20),
        name="assemble_kv",
        interpret=interpret,
    )(source_arr, *pieces)


def weight_grads_kernel(dq0_ref, dq1_ref, dkv0_ref, dkv1_ref, x_ref, gq_ref, gk_ref, gv_ref):
    x_cols = x_ref[...]
    half_q = dq0_ref.shape[0]
    d = dkv0_ref.shape[0] // 2
    gq_ref[:half_q, :] = mm(dq0_ref[...], x_cols).astype(BF16)
    gq_ref[half_q:, :] = mm(dq1_ref[...], x_cols).astype(BF16)
    for i, ref in enumerate((dkv0_ref, dkv1_ref)):
        both = mm(ref[...], x_cols).astype(BF16)
        gk_ref[i * d:(i + 1) * d, :] = both[:d]
        gv_ref[i * d:(i + 1) * d, :] = both[d:]


def weight_grads(dq_parts, dkv_parts, x_rows, interpret=False):
    n_rows, model = x_rows.shape
    cols = min(512, model)
    q_feats = 2 * dq_parts[0].shape[0]
    kv_feats = dkv_parts[0].shape[0]
    whole = lambda arr: pl.BlockSpec(arr.shape, lambda i: (0, 0))
    block = lambda feats: pl.BlockSpec((feats, cols), lambda i: (0, i))
    return pl.pallas_call(
        weight_grads_kernel,
        grid=(model // cols,),
        out_shape=tuple(jax.ShapeDtypeStruct((feats, model), BF16) for feats in (q_feats, kv_feats, kv_feats)),
        in_specs=[whole(dq_parts[0])] * 2 + [whole(dkv_parts[0])] * 2 + [block(n_rows)],
        out_specs=(block(q_feats), block(kv_feats), block(kv_feats)),
        cost_estimate=pl.CostEstimate(flops=2 * (q_feats + 2 * kv_feats) * n_rows * model, bytes_accessed=10 << 20, transcendentals=0),
        compiler_params=pltpu.CompilerParams(vmem_limit_bytes=32 << 20),
        name="weight_grads",
        interpret=interpret,
    )(*dq_parts, *dkv_parts, x_rows)


def solution(mesh, interpret=False):
    n_cp, n_tp, n_dp = mesh.shape["cp"], mesh.shape["tp"], mesh.shape["dp"]
    ring = [*range(0, n_tp, 2), *reversed(range(1, n_tp, 2))]
    hop = [(ring[i], ring[(i + 1) % n_tp]) for i in range(n_tp)]
    source = [[ring[(ring.index(z) - s) % n_tp] for z in range(n_tp)] for s in range(n_tp)]

    def swap(arr, axis, bit):
        return lax.ppermute(arr, axis, [(i, i ^ bit) for i in range(mesh.shape[axis])])

    def pick(table, idx):
        out = jnp.int32(table[0])
        for i, value in enumerate(table[1:], 1):
            out = jnp.where(idx == i, value, out)
        return out

    def device_fn(x_blk, w_query, w_key, w_value, w_out, dy_blk):
        rank = lax.axis_index("cp")
        z = lax.axis_index("tp")
        model, q_heads, d = w_query.shape
        kv_heads = w_key.shape[1]
        groups = q_heads // kv_heads
        gd = groups * d
        blk = x_blk.shape[0]
        n_rows = blk * n_tp
        rank_arr = rank.astype(jnp.int32).reshape(1)
        wqt = w_query.transpose(1, 2, 0).reshape(q_heads * d, model)
        wkt = w_key.transpose(1, 2, 0).reshape(kv_heads * d, model)
        wvt = w_value.transpose(1, 2, 0).reshape(kv_heads * d, model)
        wkvt = jnp.concatenate([wkt, wvt], axis=0)
        wo = w_out.reshape(q_heads * d, model)

        n_plane = n_dp * n_cp
        plane = lax.axis_index("dp") * n_cp + rank
        w_heads = jnp.concatenate([part for h in range(kv_heads) for part in
                                   (wqt[h * gd:(h + 1) * gd], wkt[h * d:(h + 1) * d], wvt[h * d:(h + 1) * d])], axis=0)
        n_in = w_heads.shape[0] // n_plane
        n_out = wo.shape[0] // n_plane
        w_in_piece = lax.dynamic_slice(w_heads, (plane * n_in, 0), (n_in, model))
        wo_piece = lax.dynamic_slice(wo, (plane * n_out, 0), (n_out, model))

        w_in_line = [w_in_piece]

        def offset(step):
            return pick(source[step], z) * blk

        x_rows = jnp.zeros((n_rows, model), BF16)
        qt = jnp.zeros((q_heads * d, n_rows), BF16)
        kv_blocks, kv_moved = [], []
        held = x_blk

        def cp_exchange(arr):
            near = swap(arr, "cp", 1)
            far = swap(arr, "cp", 2)
            return [arr, near, far, swap(far, "cp", 1)]

        for step in range(n_tp):
            following = lax.ppermute(held, "tp", hop) if step < n_tp - 1 else None
            if step < n_tp - 1:
                w_in_line.append(lax.ppermute(w_in_line[-1], "tp", hop))
            kv_blocks.append(mm(held, wkvt, NT).astype(BF16))
            qt = lax.dynamic_update_slice(qt, mm(wqt, held, NT).astype(BF16) * BF16(d ** -0.5), (0, offset(step)))
            x_rows = lax.dynamic_update_slice(x_rows, held, (offset(step), 0))
            if step == n_tp - 2:
                kv_moved.append(cp_exchange(jnp.stack(kv_blocks)))
            if step == n_tp - 1:
                kv_moved.append(cp_exchange(kv_blocks[-1][None]))
            if following is not None:
                following, qt, x_rows, kv_blocks[-1], kv_moved, w_in_line[:-1] = lax.optimization_barrier(
                    (following, qt, x_rows, kv_blocks[-1], kv_moved, w_in_line[:-1]))
                held = following
        dy_first, _ = lax.optimization_barrier((dy_blk, held))
        w_in_line, _ = lax.optimization_barrier((w_in_line, kv_blocks[-1]))
        w_in_line = jnp.concatenate(w_in_line, axis=0)
        w_in_full = lax.all_gather(w_in_line, ("dp", "cp"), axis=0, tiled=True)
        qt, w_in_line = lax.optimization_barrier((qt, w_in_line))
        source_arr = jnp.stack([pick(source[step], z) for step in range(n_tp)])
        pieces = [kv_moved[i][slot] for slot in range(n_cp) for i in range(2)]
        kv_all = assemble_kv(source_arr, pieces, n_rows, interpret)

        dy_rows = jnp.zeros((n_rows, model), BF16)
        dot = jnp.zeros((q_heads * d, n_rows), BF16)
        dy_held = dy_first
        fwd = []
        for step in range(n_tp):
            following = lax.ppermute(dy_held, "tp", hop) if step < n_tp - 1 else None
            dy_rows = lax.dynamic_update_slice(dy_rows, dy_held, (offset(step), 0))
            dot = lax.dynamic_update_slice(dot, mm(wo, dy_held, NT).astype(BF16), (0, offset(step)))
            if 1 <= step <= kv_heads:
                h = step - 1
                qt, kv_all, x_rows, dy_rows, dot = lax.optimization_barrier((qt, kv_all, x_rows, dy_rows, dot))
                fwd.append(attention_forward(rank_arr, qt, kv_all, h, kv_heads, n_cp, groups, d, interpret))
                if following is not None:
                    following, ot_h = lax.optimization_barrier((following, fwd[h][0]))
                    fwd[h] = (ot_h,) + tuple(fwd[h][1:])
            dy_last, dy_held = dy_held, following
        ot = jnp.concatenate([f[0] for f in fwd], axis=0)

        def exchange(arr_t):
            sent = [lax.dynamic_slice(arr_t, (0, lax.bitwise_xor(z, k) * blk), (arr_t.shape[0], blk)) for k in range(n_tp)]
            return [sent[0]] + [swap(sent[k], "tp", k) for k in range(1, n_tp)]

        def plane_order(parts, n_pieces):
            feats, rows = parts.shape[1:]
            return parts.reshape(n_tp, n_pieces, feats // n_pieces, rows).transpose(1, 0, 2, 3).reshape(n_tp * feats, rows)

        def by_arrival(parts):
            stacked = jnp.stack(parts)
            return jnp.stack([lax.dynamic_index_in_dim(stacked, lax.bitwise_xor(z, pick(source[t], z)), 0, keepdims=False)
                              for t in range(n_tp)])

        wo_piece, _ = lax.optimization_barrier((wo_piece, dy_last))
        wo_line = jnp.concatenate([wo_piece] + [swap(wo_piece, "tp", k) for k in range(1, n_tp)], axis=0)
        o_parts = exchange(ot)

        dq_parts, dkv_parts, moved, waiting = [], [], [], None
        for h in range(kv_heads):
            dqt, dkv = attention_backward(rank_arr, qt, dot, fwd[h][0], fwd[h][1], kv_all, fwd[h][2],
                                          h, kv_heads, n_cp, groups, d, interpret)
            dq_parts.append(dqt)
            part = [dkv[:, j * n_rows:(j + 1) * n_rows] for j in range(n_cp)]
            if h < kv_heads - 1:
                moved.append(exchange(dqt))
                far_parts = [swap(part[j], "cp", j) for j in range(1, n_cp)]
                waiting = (part[0], far_parts)
                if h == 0:
                    wo_line, dqt, w_in_full = lax.optimization_barrier((wo_line, dqt, w_in_full))
                    wo_full = lax.all_gather(wo_line, ("dp", "cp"), axis=0, tiled=True)
            else:
                near = swap(jnp.concatenate([part[1], part[3]], axis=1), "cp", 1)
                far_sum = part[2] + near[:, n_rows:]
                if waiting is not None:
                    far_sum, waiting = lax.optimization_barrier((far_sum, waiting))
                    own, far_parts = waiting
                    dkv_own = functools.reduce(jnp.add, far_parts, own).astype(BF16)
                    dkv_parts.append(dkv_own)
                    moved.append(exchange(jnp.concatenate([dkv_own, dqt], axis=0)))
                else:
                    moved.append(exchange(dqt))
                far = swap(far_sum, "cp", 2)
                dkv_own = (part[0] + near[:, :n_rows] + far).astype(BF16)
                dkv_parts.append(dkv_own)
                moved.append(exchange(dkv_own))
        n_early = (n_in * n_plane - dkv_parts[-1].shape[0]) // n_in
        early = [jnp.concatenate([m[k] for m in moved[:-1]], axis=0) for k in range(n_tp)]
        split = n_early * n_in * n_tp
        dx_early = mm(plane_order(by_arrival([part[:n_early * n_in] for part in early]), n_early), w_in_full[:split], TN)
        y_blk = mm(plane_order(jnp.stack(o_parts), n_plane), wo_full, TN).astype(BF16)
        last = moved[-1]
        late = [jnp.concatenate([early[k][n_early * n_in:], last[k]], axis=0) for k in range(n_tp)]
        dx_blk = (dx_early + mm(plane_order(by_arrival(late), n_plane - n_early), w_in_full[split:], TN)).astype(BF16)

        def weight_layout(grad_t):
            return grad_t.reshape(-1, d, model).transpose(2, 0, 1)[None]

        grad_wq, grad_wk, grad_wv = weight_grads(dq_parts, dkv_parts, x_rows, interpret)
        grad_wo = mm(ot, dy_rows).astype(BF16).reshape(q_heads, d, model)
        return (y_blk, dx_blk, weight_layout(grad_wq), weight_layout(grad_wk), weight_layout(grad_wv),
                grad_wo[None])

    return jax.shard_map(device_fn, mesh=mesh,
                         in_specs=(ROW_SPEC, HEAD_SPEC, HEAD_SPEC, HEAD_SPEC, OUT_W_SPEC, ROW_SPEC),
                         out_specs=(ROW_SPEC, ROW_SPEC, GRAD_SPEC, GRAD_SPEC, GRAD_SPEC, GRAD_OUT_SPEC),
                         check_vma=False)
```

```python
import functools

import jax
import jax.numpy as jnp
from jax import lax
from jax.experimental import pallas as pl
from jax.experimental.pallas import tpu as pltpu
from jax.sharding import PartitionSpec as P


ROW_SPEC = P(("dp", "cp", "tp"), None)
HEAD_SPEC = P(None, "tp", None)
OUT_W_SPEC = P("tp", None, None)
GRAD_SPEC = P(("dp", "cp"), None, "tp", None)
GRAD_OUT_SPEC = P(("dp", "cp"), "tp", None, None)
TN = (((0,), (0,)), ((), ()))
NT = (((1,), (1,)), ((), ()))
F32 = jnp.float32
BF16 = jnp.bfloat16


def mm(lhs, rhs, dims=(((1,), (0,)), ((), ()))):
    return lax.dot_general(lhs, rhs, dims, preferred_element_type=F32)


def chunk_offset(chunk, rank, n_shards, half):
    shard = jnp.where(chunk < n_shards, chunk, 2 * n_shards - 1 - chunk)
    upper = jnp.where(chunk < n_shards, 0, half)
    return pl.multiple_of(lax.bitwise_xor(shard, rank) * (2 * half) + upper, half)


def forward_kernel(n_shards, groups, d, half, h, kv_heads, rank_ref, qt_ref, kv_ref, ot_ref, lse_ref, kt_ref, q_pad, vt_s, m_s, l_s, acc_s):
    rank = rank_ref[0]
    kw = kv_heads * d
    sub = half // 2
    q_pad[...] = jnp.zeros_like(q_pad)
    for g in range(groups):
        q_pad[g, h * d:(h + 1) * d, :] = qt_ref[(h * groups + g) * d:(h * groups + g + 1) * d, :]

    def transpose_chunk(i, carry):
        rows = pl.ds(pl.multiple_of(i * half, half), half)
        kt_ref[:, rows] = kv_ref[rows, :kw].T[h * d:(h + 1) * d, :]
        vt_s[:, rows] = kv_ref[rows, kw:].T[h * d:(h + 1) * d, :]
        return carry

    lax.fori_loop(0, kv_ref.shape[0] // half, transpose_chunk, 0)

    def update(g, q_start, q_lo, q_len, k_off, k_len, masked):
        cols = slice(q_lo, q_lo + q_len)
        scores = mm(kv_ref[pl.ds(k_off, k_len), :kw], q_pad[g, :, q_start + q_lo:q_start + q_lo + q_len])
        if masked:
            k_id = lax.broadcasted_iota(jnp.int32, scores.shape, 0)
            q_id = lax.broadcasted_iota(jnp.int32, scores.shape, 1)
            scores = jnp.where(q_id >= k_id, scores, -jnp.inf)
        m_old = m_s[g:g + 1, cols]
        m_new = jnp.maximum(m_old, jnp.max(scores, axis=0, keepdims=True))
        prob = jnp.exp(scores - m_new)
        factor = jnp.exp(m_old - m_new)
        m_s[g:g + 1, cols] = m_new
        l_s[g:g + 1, cols] = l_s[g:g + 1, cols] * factor + jnp.sum(prob, axis=0, keepdims=True)
        pv = mm(vt_s[:, pl.ds(k_off, k_len)], prob.astype(BF16))
        acc_s[g * d:(g + 1) * d, cols] = acc_s[g * d:(g + 1) * d, cols] * factor + pv

    for q_half in range(2):
        q_start = q_half * half
        n_full = rank if q_half == 0 else 2 * n_shards - 1 - rank
        m_s[...] = jnp.full_like(m_s, -jnp.inf)
        l_s[...] = jnp.zeros_like(l_s)
        acc_s[...] = jnp.zeros_like(acc_s)
        off = chunk_offset(n_full, rank, n_shards, half)
        for g in range(groups):
            update(g, q_start, 0, half, off, sub, True)
        for g in range(groups):
            update(g, q_start, sub, sub, pl.multiple_of(off + sub, sub), sub, True)

        def full_block(chunk, carry):
            k_off = chunk_offset(chunk, rank, n_shards, half)
            for g in range(groups):
                update(g, q_start, 0, half, k_off, half, False)
            return carry

        lax.fori_loop(0, n_full, full_block, 0)
        for g in range(groups):
            l_row = l_s[g:g + 1, :]
            ot_ref[g * d:(g + 1) * d, q_start:q_start + half] = (acc_s[g * d:(g + 1) * d, :] / l_row).astype(BF16)
            lse_ref[g:g + 1, q_start:q_start + half] = m_s[g:g + 1, :] + jnp.log(l_row)


def backward_kernel(n_shards, groups, d, half, h, kv_heads, rank_ref, qt_ref, dot_ref, ot_ref, lse_ref, kv_ref, kt_ref,
                    dqt_ref, dkv_ref, q_pad, do_pad, delta_s, dq_s):
    rank = rank_ref[0]
    kw = kv_heads * d
    sub = half // 2
    q_pad[...] = jnp.zeros_like(q_pad)
    do_pad[...] = jnp.zeros_like(do_pad)
    for g in range(groups):
        rows = slice(g * d, (g + 1) * d)
        full = slice((h * groups + g) * d, (h * groups + g + 1) * d)
        q_pad[g, h * d:(h + 1) * d, :] = qt_ref[full, :]
        do_pad[g, h * d:(h + 1) * d, :] = dot_ref[full, :]
        delta_s[g:g + 1, :] = jnp.sum(dot_ref[full, :].astype(F32) * ot_ref[rows, :].astype(F32), axis=0, keepdims=True)
    dkv_ref[...] = jnp.zeros_like(dkv_ref)

    def update(q_start, q_lo, q_len, k_off, k_len, masked):
        lo = q_start + q_lo
        cols = slice(lo, lo + q_len)
        k_blk = kv_ref[pl.ds(k_off, k_len), :kw]
        v_blk = kv_ref[pl.ds(k_off, k_len), kw:]
        dk_sum, dv_sum = None, None
        for g in range(groups):
            rows = slice(g * d, (g + 1) * d)
            full = slice((h * groups + g) * d, (h * groups + g + 1) * d)
            scores = mm(k_blk, q_pad[g, :, cols])
            prob = jnp.exp(scores - lse_ref[g:g + 1, cols])
            if masked:
                k_id = lax.broadcasted_iota(jnp.int32, scores.shape, 0)
                q_id = lax.broadcasted_iota(jnp.int32, scores.shape, 1)
                prob = jnp.where(q_id >= k_id, prob, 0.0)
            d_prob = mm(v_blk, do_pad[g, :, cols])
            d_score = (prob * (d_prob - delta_s[g:g + 1, cols])).astype(BF16)
            dv = mm(dot_ref[full, cols], prob.astype(BF16), NT)
            dk = mm(qt_ref[full, cols], d_score, NT)
            dk_sum = dk if dk_sum is None else dk_sum + dk
            dv_sum = dv if dv_sum is None else dv_sum + dv
            dq_s[rows, q_lo:q_lo + q_len] += mm(kt_ref[:, pl.ds(k_off, k_len)], d_score)
        dkv_ref[:d, pl.ds(k_off, k_len)] += dk_sum
        dkv_ref[d:, pl.ds(k_off, k_len)] += dv_sum

    for q_half in range(2):
        q_start = q_half * half
        n_full = rank if q_half == 0 else 2 * n_shards - 1 - rank
        dq_s[...] = jnp.zeros_like(dq_s)
        off = chunk_offset(n_full, rank, n_shards, half)
        update(q_start, 0, half, off, sub, True)
        update(q_start, sub, sub, pl.multiple_of(off + sub, sub), sub, True)

        def full_block(chunk, carry):
            update(q_start, 0, half, chunk_offset(chunk, rank, n_shards, half), half, False)
            return carry

        lax.fori_loop(0, n_full, full_block, 0)
        dqt_ref[:, q_start:q_start + half] = (dq_s[...] * (d ** -0.5)).astype(BF16)


VMEM = pl.BlockSpec(memory_space=pltpu.VMEM)
SMEM = pl.BlockSpec(memory_space=pltpu.SMEM)


def attention_forward(rank_arr, qt, kv_all, h, kv_heads, n_shards, groups, d, interpret=False):
    n_rows = qt.shape[1]
    half = n_rows // 2
    kw = kv_all.shape[1] // 2
    pairs = groups * n_rows * n_rows * n_shards // 2
    return pl.pallas_call(
        functools.partial(forward_kernel, n_shards, groups, d, half, h, kv_heads),
        out_shape=(jax.ShapeDtypeStruct((groups * d, n_rows), BF16), jax.ShapeDtypeStruct((groups, n_rows), F32),
                   jax.ShapeDtypeStruct((d, kv_all.shape[0]), BF16)),
        in_specs=[SMEM, VMEM, VMEM],
        out_specs=(VMEM, VMEM, VMEM),
        scratch_shapes=[pltpu.VMEM((groups, kw, n_rows), BF16), pltpu.VMEM((d, kv_all.shape[0]), BF16),
                        pltpu.VMEM((groups, half), F32), pltpu.VMEM((groups, half), F32), pltpu.VMEM((groups * d, half), F32)],
        cost_estimate=pl.CostEstimate(flops=32 * d * pairs, bytes_accessed=6 << 20, transcendentals=pairs),
        compiler_params=pltpu.CompilerParams(vmem_limit_bytes=40 << 20),
        interpret=interpret,
    )(rank_arr, qt, kv_all)


def attention_backward(rank_arr, qt, dot, ot, lse, kv_all, kt, h, kv_heads, n_shards, groups, d, interpret=False):
    n_rows = qt.shape[1]
    half = n_rows // 2
    kw = kv_all.shape[1] // 2
    pairs = groups * n_rows * n_rows * n_shards // 2
    return pl.pallas_call(
        functools.partial(backward_kernel, n_shards, groups, d, half, h, kv_heads),
        out_shape=(jax.ShapeDtypeStruct((groups * d, n_rows), BF16), jax.ShapeDtypeStruct((2 * d, kv_all.shape[0]), F32)),
        in_specs=[SMEM] + [VMEM] * 6,
        out_specs=(VMEM, VMEM),
        scratch_shapes=[pltpu.VMEM((groups, kw, n_rows), BF16), pltpu.VMEM((groups, kw, n_rows), BF16),
                        pltpu.VMEM((groups, n_rows), F32), pltpu.VMEM((groups * d, half), F32)],
        cost_estimate=pl.CostEstimate(flops=40 * d * pairs, bytes_accessed=8 << 20, transcendentals=pairs),
        compiler_params=pltpu.CompilerParams(vmem_limit_bytes=40 << 20),
        interpret=interpret,
    )(rank_arr, qt, dot, ot, lse, kv_all, kt)


def assemble_kernel(n_rows, source_ref, *refs):
    out_ref = refs[-1]
    n_slots = (len(refs) - 1) // 2
    for slot in range(n_slots):
        arrived = 0
        for ref in (refs[2 * slot], refs[2 * slot + 1]):
            for i in range(ref.shape[0]):
                blk = ref.shape[1]
                start = pl.multiple_of(slot * n_rows + source_ref[arrived] * blk, blk)
                out_ref[pl.ds(start, blk), :] = ref[i]
                arrived += 1


def assemble_kv(source_arr, pieces, n_rows, interpret=False):
    n_slots = len(pieces) // 2
    width = pieces[0].shape[2]
    return pl.pallas_call(
        functools.partial(assemble_kernel, n_rows),
        out_shape=jax.ShapeDtypeStruct((n_slots * n_rows, width), BF16),
        in_specs=[SMEM] + [VMEM] * len(pieces),
        out_specs=VMEM,
        cost_estimate=pl.CostEstimate(flops=1 << 20, bytes_accessed=4 * n_slots * n_rows * width, transcendentals=0),
        compiler_params=pltpu.CompilerParams(vmem_limit_bytes=16 << 20),
        name="assemble_kv",
        interpret=interpret,
    )(source_arr, *pieces)


def weight_grads_kernel(dkv0_ref, dkv1_ref, x_ref, gk_ref, gv_ref):
    x_cols = x_ref[...]
    d = dkv0_ref.shape[0] // 2
    for i, ref in enumerate((dkv0_ref, dkv1_ref)):
        both = mm(ref[...], x_cols).astype(BF16)
        gk_ref[i * d:(i + 1) * d, :] = both[:d]
        gv_ref[i * d:(i + 1) * d, :] = both[d:]


def weight_grads(dkv_parts, x_rows, interpret=False):
    n_rows, model = x_rows.shape
    cols = min(512, model)
    kv_feats = dkv_parts[0].shape[0]
    whole = lambda arr: pl.BlockSpec(arr.shape, lambda i: (0, 0))
    block = lambda feats: pl.BlockSpec((feats, cols), lambda i: (0, i))
    return pl.pallas_call(
        weight_grads_kernel,
        grid=(model // cols,),
        out_shape=tuple(jax.ShapeDtypeStruct((feats, model), BF16) for feats in (kv_feats, kv_feats)),
        in_specs=[whole(dkv_parts[0])] * 2 + [block(n_rows)],
        out_specs=(block(kv_feats), block(kv_feats)),
        cost_estimate=pl.CostEstimate(flops=4 * kv_feats * n_rows * model, bytes_accessed=10 << 20, transcendentals=0),
        compiler_params=pltpu.CompilerParams(vmem_limit_bytes=32 << 20),
        name="weight_grads",
        interpret=interpret,
    )(*dkv_parts, x_rows)


def solution(mesh, interpret=False):
    n_cp, n_tp, n_dp = mesh.shape["cp"], mesh.shape["tp"], mesh.shape["dp"]
    ring = [*range(0, n_tp, 2), *reversed(range(1, n_tp, 2))]
    hop = [(ring[i], ring[(i + 1) % n_tp]) for i in range(n_tp)]
    source = [[ring[(ring.index(z) - s) % n_tp] for z in range(n_tp)] for s in range(n_tp)]

    def swap(arr, axis, bit):
        return lax.ppermute(arr, axis, [(i, i ^ bit) for i in range(mesh.shape[axis])])

    def pick(table, idx):
        out = jnp.int32(table[0])
        for i, value in enumerate(table[1:], 1):
            out = jnp.where(idx == i, value, out)
        return out

    def device_fn(x_blk, w_query, w_key, w_value, w_out, dy_blk):
        rank = lax.axis_index("cp")
        z = lax.axis_index("tp")
        model, q_heads, d = w_query.shape
        kv_heads = w_key.shape[1]
        groups = q_heads // kv_heads
        gd = groups * d
        blk = x_blk.shape[0]
        n_rows = blk * n_tp
        rank_arr = rank.astype(jnp.int32).reshape(1)
        wqt = w_query.transpose(1, 2, 0).reshape(q_heads * d, model)
        wkt = w_key.transpose(1, 2, 0).reshape(kv_heads * d, model)
        wvt = w_value.transpose(1, 2, 0).reshape(kv_heads * d, model)
        wkvt = jnp.concatenate([wkt, wvt], axis=0)
        wo = w_out.reshape(q_heads * d, model)

        n_plane = n_dp * n_cp
        plane = lax.axis_index("dp") * n_cp + rank
        w_heads = jnp.concatenate([part for h in range(kv_heads) for part in
                                   (wqt[h * gd:(h + 1) * gd], wkt[h * d:(h + 1) * d], wvt[h * d:(h + 1) * d])], axis=0)
        n_in = w_heads.shape[0] // n_plane
        n_out = wo.shape[0] // n_plane
        w_in_piece = lax.dynamic_slice(w_heads, (plane * n_in, 0), (n_in, model))
        wo_piece = lax.dynamic_slice(wo, (plane * n_out, 0), (n_out, model))

        w_in_line = [w_in_piece]

        def offset(step):
            return pick(source[step], z) * blk

        x_rows = jnp.zeros((n_rows, model), BF16)
        qt = jnp.zeros((q_heads * d, n_rows), BF16)
        kv_blocks, kv_moved = [], []
        held = x_blk

        def cp_exchange(arr):
            near = swap(arr, "cp", 1)
            far = swap(arr, "cp", 2)
            return [arr, near, far, swap(far, "cp", 1)]

        for step in range(n_tp):
            following = lax.ppermute(held, "tp", hop) if step < n_tp - 1 else None
            if step < n_tp - 1:
                w_in_line.append(lax.ppermute(w_in_line[-1], "tp", hop))
            kv_blocks.append(mm(held, wkvt, NT).astype(BF16))
            qt = lax.dynamic_update_slice(qt, mm(wqt, held, NT).astype(BF16) * BF16(d ** -0.5), (0, offset(step)))
            x_rows = lax.dynamic_update_slice(x_rows, held, (offset(step), 0))
            if step == n_tp - 2:
                kv_moved.append(cp_exchange(jnp.stack(kv_blocks)))
            if step == n_tp - 1:
                kv_moved.append(cp_exchange(kv_blocks[-1][None]))
            if following is not None:
                following, qt, x_rows, kv_blocks[-1], kv_moved, w_in_line[:-1] = lax.optimization_barrier(
                    (following, qt, x_rows, kv_blocks[-1], kv_moved, w_in_line[:-1]))
                held = following
        dy_first, _ = lax.optimization_barrier((dy_blk, held))
        w_in_line, _ = lax.optimization_barrier((w_in_line, kv_blocks[-1]))
        w_in_line = jnp.concatenate(w_in_line, axis=0)
        w_in_full = lax.all_gather(w_in_line, ("dp", "cp"), axis=0, tiled=True)
        qt, w_in_line = lax.optimization_barrier((qt, w_in_line))
        source_arr = jnp.stack([pick(source[step], z) for step in range(n_tp)])
        pieces = [kv_moved[i][slot] for slot in range(n_cp) for i in range(2)]
        kv_all = assemble_kv(source_arr, pieces, n_rows, interpret)

        dy_rows = jnp.zeros((n_rows, model), BF16)
        dot = jnp.zeros((q_heads * d, n_rows), BF16)
        dy_held = dy_first
        fwd = []
        for step in range(n_tp):
            following = lax.ppermute(dy_held, "tp", hop) if step < n_tp - 1 else None
            dy_rows = lax.dynamic_update_slice(dy_rows, dy_held, (offset(step), 0))
            dot = lax.dynamic_update_slice(dot, mm(wo, dy_held, NT).astype(BF16), (0, offset(step)))
            if 1 <= step <= kv_heads:
                h = step - 1
                qt, kv_all, x_rows, dy_rows, dot = lax.optimization_barrier((qt, kv_all, x_rows, dy_rows, dot))
                fwd.append(attention_forward(rank_arr, qt, kv_all, h, kv_heads, n_cp, groups, d, interpret))
                if following is not None:
                    following, ot_h = lax.optimization_barrier((following, fwd[h][0]))
                    fwd[h] = (ot_h,) + tuple(fwd[h][1:])
            dy_last, dy_held = dy_held, following
        ot = jnp.concatenate([f[0] for f in fwd], axis=0)

        def exchange(arr_t):
            sent = [lax.dynamic_slice(arr_t, (0, lax.bitwise_xor(z, k) * blk), (arr_t.shape[0], blk)) for k in range(n_tp)]
            return [sent[0]] + [swap(sent[k], "tp", k) for k in range(1, n_tp)]

        def plane_order(parts, n_pieces):
            feats, rows = parts.shape[1:]
            return parts.reshape(n_tp, n_pieces, feats // n_pieces, rows).transpose(1, 0, 2, 3).reshape(n_tp * feats, rows)

        def by_arrival(parts):
            stacked = jnp.stack(parts)
            return jnp.stack([lax.dynamic_index_in_dim(stacked, lax.bitwise_xor(z, pick(source[t], z)), 0, keepdims=False)
                              for t in range(n_tp)])

        wo_piece, _ = lax.optimization_barrier((wo_piece, dy_last))
        wo_line = jnp.concatenate([wo_piece] + [swap(wo_piece, "tp", k) for k in range(1, n_tp)], axis=0)
        o_parts = exchange(ot)

        dq_parts, dkv_parts, moved, waiting = [], [], [], None
        for h in range(kv_heads):
            dqt, dkv = attention_backward(rank_arr, qt, dot, fwd[h][0], fwd[h][1], kv_all, fwd[h][2],
                                          h, kv_heads, n_cp, groups, d, interpret)
            dq_parts.append(dqt)
            part = [dkv[:, j * n_rows:(j + 1) * n_rows] for j in range(n_cp)]
            if h < kv_heads - 1:
                moved.append(exchange(dqt))
                far_parts = [swap(part[j], "cp", j) for j in range(1, n_cp)]
                waiting = (part[0], far_parts)
                if h == 0:
                    wo_line, dqt, w_in_full = lax.optimization_barrier((wo_line, dqt, w_in_full))
                    wo_full = lax.all_gather(wo_line, ("dp", "cp"), axis=0, tiled=True)
            else:
                near = swap(jnp.concatenate([part[1], part[3]], axis=1), "cp", 1)
                far_sum = part[2] + near[:, n_rows:]
                if waiting is not None:
                    far_sum, waiting = lax.optimization_barrier((far_sum, waiting))
                    own, far_parts = waiting
                    dkv_own = functools.reduce(jnp.add, far_parts, own).astype(BF16)
                    dkv_parts.append(dkv_own)
                    moved.append(exchange(jnp.concatenate([dkv_own, dqt], axis=0)))
                else:
                    moved.append(exchange(dqt))
                far = swap(far_sum, "cp", 2)
                dkv_own = (part[0] + near[:, :n_rows] + far).astype(BF16)
                dkv_parts.append(dkv_own)
                moved.append(exchange(dkv_own))
        n_early = (n_in * n_plane - dkv_parts[-1].shape[0]) // n_in
        early = [jnp.concatenate([m[k] for m in moved[:-1]], axis=0) for k in range(n_tp)]
        split = n_early * n_in * n_tp
        dx_early = mm(plane_order(by_arrival([part[:n_early * n_in] for part in early]), n_early), w_in_full[:split], TN)
        y_blk = mm(plane_order(jnp.stack(o_parts), n_plane), wo_full, TN).astype(BF16)
        last = moved[-1]
        late = [jnp.concatenate([early[k][n_early * n_in:], last[k]], axis=0) for k in range(n_tp)]
        dx_blk = (dx_early + mm(plane_order(by_arrival(late), n_plane - n_early), w_in_full[split:], TN)).astype(BF16)

        def weight_layout(grad_t):
            return grad_t.reshape(-1, d, model).transpose(2, 0, 1)[None]

        grad_wk, grad_wv = weight_grads(dkv_parts, x_rows, interpret)
        grad_wq = mm(jnp.concatenate(dq_parts, axis=0), x_rows).astype(BF16)
        grad_wo = mm(ot, dy_rows).astype(BF16).reshape(q_heads, d, model)
        return (y_blk, dx_blk, weight_layout(grad_wq), weight_layout(grad_wk), weight_layout(grad_wv),
                grad_wo[None])

    return jax.shard_map(device_fn, mesh=mesh,
                         in_specs=(ROW_SPEC, HEAD_SPEC, HEAD_SPEC, HEAD_SPEC, OUT_W_SPEC, ROW_SPEC),
                         out_specs=(ROW_SPEC, ROW_SPEC, GRAD_SPEC, GRAD_SPEC, GRAD_SPEC, GRAD_OUT_SPEC),
                         check_vma=False)
```
